256 devices in a mesh: sec: 16 (over x_lo, y, core), strip: 16 (over z, x_hi).
Axes of the slice: x: 4 (x_hi: 2, x_lo: 2; x = x_hi * 2 + x_lo), y: 4, z: 8, core: 2. Of those that a mesh axis runs over, the one named last changes fastest.
Arguments:
- images: bfloat16 [16, 2048, 1024], P('sec', 'strip'), may hold values from -6 to 6
- row_weights: float32 [16, 4, 2048], P('sec', None, 'strip'), may hold values from 0.05 to 0.5
- row_shift: int32 [16, 16], P('sec', 'strip'), may hold values from -4 to 4
- col_weights: bfloat16 [16, 4, 1024], P('sec'), may hold values from 0.049804688 to 0.5
- col_shift: int32 [16], P('sec'), may hold values from -32 to 32
- pair_on: int32 [16, 3], replicated, may hold values 0 or 1
Outputs:
- grad_warped: float32 [16, 2048, 1024], P('sec', 'strip')
- displacement: float32 [2, 16, 2048, 1024], P(None, 'sec', 'strip')
The draws below stay inside these ranges and needn't reach their ends.
All inputs are finite; a program needn't handle non-finite values.
Results may differ from the reference program's by a relative error of at most 0.0047.
Values may be sent and summed in bfloat16 or wider, within the bound.
No kernel may reach another device: no remote copies, remote signals or barrier semaphores. Data moves between devices by JAX's collectives and lax.ppermute only.
A program may use at most 64 MiB of HBM per device.

```python
import jax
import jax.numpy as jnp
from jax import lax

ROWS_DEV = 128
WIDTH = 1024
TAP_COUNT = 4
MAX_SHIFT = 4
COL_REACH = 32
RADIUS = 4
PAIR_REACH = 3
SECTIONS = 16
HEIGHT = 2048
STRIPS = 16


def with_ends(result, own_key, smallest, top_value):
    longest = result.shape.index(max(result.shape))
    spots = []
    for shift in (0, 1):
        where = [jax.random.randint(jax.random.fold_in(own_key, axis), (), 0, length) for axis, length in enumerate(result.shape)]
        where[longest] = (where[longest] + shift) % result.shape[longest]
        spots.append(tuple(where))
    return result.at[spots[0]].set(smallest).at[spots[1]].set(top_value)


def level_of(key, extent, split, low, high):
    def one(axis_at, blocks):
        steps = jax.random.uniform(jax.random.fold_in(jax.random.fold_in(key, 6), axis_at), (blocks,), jnp.float32, low / len(split), high / len(split))
        return jnp.repeat(jnp.exp(steps), extent[axis_at] // blocks).reshape((-1,) + (1,) * (len(extent) - axis_at - 1))

    level = one(*split[0])
    for cut in split[1:]:
        level = level * one(*cut)
    return level


def normal_values(rng, dims, deviation, limit, cuts=(), kind=jnp.bfloat16):
    entries = jax.random.normal(rng, dims, jnp.float32) * deviation
    if len(cuts) > 0:
        entries = level_of(rng, dims, cuts, -0.22, 0.18) * entries
    return jnp.clip(entries, min=-limit, max=limit).astype(kind)


def setup_inputs(seed: int = 0) -> dict:
    key_list = jax.random.split(jax.random.key(seed), 7)
    return {
        "images": normal_values(key_list[0], (SECTIONS, HEIGHT, WIDTH), 1.0, 6.0, ((0, 16), (1, 16))),
        "row_weights": jnp.clip(0.05 + 0.45 * jax.random.uniform(key_list[1], (SECTIONS, TAP_COUNT, HEIGHT), jnp.float32) ** level_of(key_list[1], (SECTIONS, TAP_COUNT, HEIGHT), ((0, 16), (2, 16)), -0.2, 0.2), 0.05, 0.5),
        "row_shift": with_ends(jax.random.randint(key_list[2], (SECTIONS, STRIPS), 0 - MAX_SHIFT, MAX_SHIFT + 1), jax.random.fold_in(key_list[2], 1), 0 - MAX_SHIFT, MAX_SHIFT).astype(jnp.int32),
        "col_weights": jnp.clip(0.049804688 + 0.4501953 * jax.random.uniform(key_list[3], (SECTIONS, TAP_COUNT, WIDTH), jnp.float32) ** level_of(key_list[3], (SECTIONS, TAP_COUNT, WIDTH), ((0, 16),), -0.2, 0.2), 0.049804688, 0.5).astype(jnp.bfloat16),
        "col_shift": with_ends(jax.random.randint(key_list[4], (SECTIONS,), 0 - COL_REACH, COL_REACH + 1), jax.random.fold_in(key_list[4], 1), 0 - COL_REACH, COL_REACH).astype(jnp.int32),
        "pair_on": with_ends((jax.random.randint(key_list[5], (SECTIONS, PAIR_REACH), 0, 4) < 3).astype(jnp.int32), jax.random.fold_in(key_list[5], 1), 0, 1),
    }


variance_bias = 0.25

def box_sum(field):
    size_box = 2 * RADIUS + 1
    row_count = field.shape[-2]
    col_count = field.shape[-1]
    widths = [(0, 0)] * (field.ndim - 2) + [(RADIUS, RADIUS), (RADIUS, RADIUS)]
    padded = jnp.pad(field, widths)
    across = padded[..., 0:row_count, :]
    for step_row in range(1, size_box):
        across = across + padded[..., step_row:step_row + row_count, :]
    running = across[..., 0:col_count]
    for step_col in range(1, size_box):
        running = running + across[..., step_col:step_col + col_count]
    return running

def warp_section(section_items):
    image, weights, shifts, column_taps, column_shift = section_items
    source_depth = MAX_SHIFT + 2
    padded = jnp.pad(image, ((source_depth, source_depth), (0, 0)))
    shift_rows = jnp.repeat(shifts.astype(jnp.int32), ROWS_DEV)
    base_rows = jnp.arange(HEIGHT, dtype=jnp.int32) + shift_rows + (source_depth - 1)
    running = jnp.zeros((HEIGHT, WIDTH), jnp.float32)
    for tap_index in range(TAP_COUNT):
        taken = jnp.take(padded, (base_rows + tap_index).astype(jnp.int32), axis=0)
        running = running + weights[tap_index][:, None].astype(jnp.float32) * taken.astype(jnp.float32)
    row_warped = running.astype(jnp.bfloat16)
    row_ids = lax.broadcasted_iota(jnp.int32, (WIDTH, WIDTH), 0)
    col_ids = lax.broadcasted_iota(jnp.int32, (WIDTH, WIDTH), 1)
    offsets = row_ids - col_ids - column_shift.astype(jnp.int32) + 1
    matrix = jnp.zeros((WIDTH, WIDTH), column_taps.dtype)
    for tap_index in range(TAP_COUNT):
        matrix = jnp.where(offsets == tap_index, column_taps[tap_index][None, :], matrix)
    return jnp.dot(row_warped, matrix, preferred_element_type=jnp.float32).astype(jnp.bfloat16)

def pair_grads(left_field, right_field, weight):
    box_cells = float((2 * RADIUS + 1) ** 2)
    mean_left = box_sum(left_field) / box_cells
    mean_right = box_sum(right_field) / box_cells
    var_left = box_sum(left_field * left_field) / box_cells - mean_left * mean_left + variance_bias
    var_right = box_sum(right_field * right_field) / box_cells - mean_right * mean_right + variance_bias
    covariance = box_sum(left_field * right_field) / box_cells - mean_left * mean_right
    denom_root = jnp.sqrt(var_left * var_right)
    ncc_value = covariance / denom_root
    g_cov = -weight / denom_root
    g_left = weight * ncc_value / (2.0 * var_left)
    g_right = weight * ncc_value / (2.0 * var_right)
    h_left = -g_cov * mean_right - 2.0 * g_left * mean_left
    h_right = -g_cov * mean_left - 2.0 * g_right * mean_right
    boxed_cov = box_sum(g_cov)
    grad_left = (box_sum(h_left) + 2.0 * left_field * box_sum(g_left) + right_field * boxed_cov) / box_cells
    grad_right = (box_sum(h_right) + 2.0 * right_field * box_sum(g_right) + left_field * boxed_cov) / box_cells
    return (grad_left, grad_right)

def displace(section_items):
    field, grads = section_items
    field_wide = field.astype(jnp.float32)
    rows_padded = jnp.pad(field_wide, ((1, 1), (0, 0)))
    slope_rows = (rows_padded[2:] - rows_padded[:-2]) * 0.5
    cols_padded = jnp.pad(field_wide, ((0, 0), (1, 1)))
    slope_cols = (cols_padded[:, 2:] - cols_padded[:, :-2]) * 0.5
    products = jnp.stack([grads * slope_rows, grads * slope_cols])
    return -box_sum(products) / 9.0

def reference(images, row_weights, row_shift, col_weights, col_shift, pair_on):
    warped = lax.map(warp_section, (images, row_weights, row_shift, col_weights, col_shift))
    grads = jnp.zeros((SECTIONS, HEIGHT, WIDTH), jnp.float32)
    for distance in range(1, PAIR_REACH + 1):
        pair_count = SECTIONS - distance

        def one_pair(pair_items):
            left_img, right_img, weight = pair_items
            return pair_grads(left_img.astype(jnp.float32), right_img.astype(jnp.float32), weight)
        grad_left, grad_right = lax.map(one_pair, (warped[:pair_count], warped[distance:], pair_on[:pair_count, distance - 1].astype(jnp.float32)))
        grads = grads.at[:pair_count].add(grad_left)
        grads = grads.at[distance:].add(grad_right)
    displacement = lax.map(displace, (warped, grads))
    return (grads, jnp.transpose(displacement, (1, 0, 2, 3)))
```

```python
import functools

import jax
import jax.numpy as jnp
from jax import lax
from jax.experimental import pallas as pl
from jax.experimental.pallas import tpu as pltpu
from jax.sharding import PartitionSpec as P

TAPS = 4
HALO = 12
STEPS = 19
SUBS = 8
EXT = STEPS * SUBS
TILES = 8
CELLS = 81.0
F32 = jnp.float32
BF16 = jnp.bfloat16
VMEM = pl.BlockSpec(memory_space=pltpu.VMEM)
SMEM = pl.BlockSpec(memory_space=pltpu.SMEM)
EDGE = 24
BLOCK = 32


def window_sums(seq, width):
    count = len(seq) - width + 1
    out = [None] * count
    for base in range(0, count, width):
        suffix = [None] * width
        suffix[width - 1] = seq[base + width - 1]
        for i in range(width - 2, -1, -1):
            suffix[i] = seq[base + i] + suffix[i + 1]
        prefix = None
        for i in range(width):
            if base + i >= count:
                break
            if i == 0:
                out[base] = suffix[0]
            else:
                nxt = seq[base + width + i - 1]
                prefix = nxt if prefix is None else prefix + nxt
                out[base + i] = suffix[i] + prefix
    return out


def row_window(steps):
    low = [pltpu.roll(v, 1, 0) for v in steps[-4:]]
    high = [pltpu.roll(v, SUBS - 1, 0) for v in steps[:4]]
    return window_sums(low + steps + high, 9)


def col_window(tiles, first_lane, last_lane):
    zero = jnp.zeros_like(tiles[0])
    low = [jnp.where(first_lane, zero, pltpu.roll(v, 1, 1)) for v in tiles[4:]]
    high = [jnp.where(last_lane, zero, pltpu.roll(v, 127, 1)) for v in tiles[:4]]
    seq = low + tiles + high
    suffix = [None] * 8
    suffix[7] = seq[7]
    for i in range(6, -1, -1):
        suffix[i] = seq[i] + suffix[i + 1]
    out = []
    prefix = None
    for i in range(8):
        prefix = seq[8 + i] if prefix is None else prefix + seq[8 + i]
        out.append(suffix[i] + prefix)
    return out


def steps_of(value):
    return [value[8 * k : 8 * k + 8] for k in range(STEPS)]


def lanes():
    lane = lax.broadcasted_iota(jnp.int32, (8, 128), 1)
    return lane == 0, lane == 127


def put_rows(ref, tile, values):
    for k, v in enumerate(values):
        ref[tile, 8 * k : 8 * k + 8, :] = v


def get_tiles(ref, at):
    return [ref[m, pl.ds(at, 8), :] for m in range(TILES)]


def split3(value):
    hi = value.astype(BF16).astype(F32)
    rest = value - hi
    mid = rest.astype(BF16).astype(F32)
    return hi, mid, rest - mid


def prep_kernel(shift_ref, img_ref, weights_ref, up_ref, down_ref, own_ref):
    up_ref[0:EDGE, :] = img_ref[128 - EDGE : 128, :]
    down_ref[0:EDGE, :] = img_ref[0:EDGE, :]
    shift = jnp.full((1, 128), shift_ref[0, 0], jnp.int32).astype(F32)
    lane = lax.broadcasted_iota(jnp.int32, (8, 128), 1)
    row = lax.broadcasted_iota(jnp.int32, (8, 128), 0)
    zero = jnp.zeros((8, 128), F32)
    for tap in range(TAPS):
        line = jnp.broadcast_to(weights_ref[tap : tap + 1, :], (8, 128))
        hi, mid, lo = split3(pltpu.roll(line, HALO, 1))
        full = jnp.where(row == 0, hi, jnp.where(row == 1, mid, jnp.where(row == 2, lo, zero)))
        if tap == 0:
            full = jnp.where(row == 3, jnp.broadcast_to(shift, (8, 128)), full)
        at = 256 * tap
        wrapped = jnp.where(lane < HALO, full, zero).astype(BF16)
        own_ref[:, at : at + 128] = jnp.where(lane >= HALO, full, zero).astype(BF16)
        own_ref[:, at + 128 : at + 256] = wrapped
        up_ref[EDGE:BLOCK, at : at + 128] = wrapped
        up_ref[EDGE:BLOCK, at + 128 : at + 256] = zero.astype(BF16)
        down_ref[EDGE:BLOCK, at : at + 128] = zero.astype(BF16)
        down_ref[EDGE:BLOCK, at + 128 : at + 256] = jnp.where(
            (lane >= HALO) & (lane < 2 * HALO), full, zero
        ).astype(BF16)


def matrix_kernel(shift_ref, weights_ref, out_ref):
    shift = shift_ref[0]
    base = lax.broadcasted_iota(jnp.int32, (16, 128), 0) - 8 * lax.broadcasted_iota(
        jnp.int32, (16, 128), 1
    )
    for m in range(TILES):
        taps = [
            jnp.broadcast_to(weights_ref[t : t + 1, 128 * m : 128 * m + 128].astype(F32), (16, 128))
            for t in range(TAPS)
        ]

        def body(step, carry):
            offset = base - (m + shift - 1 - 16 * step)
            value = jnp.zeros((16, 128), F32)
            for t in range(TAPS):
                value = jnp.where(offset == t, taps[t], value)
            out_ref[pl.ds(pl.multiple_of(16 * step, 16), 16), 128 * m : 128 * m + 128] = value.astype(BF16)
            return carry

        lax.fori_loop(0, 64, body, 0, unroll=8)


def warp_kernel(img_ref, low_ref, high_ref, own_ref, matrix_ref, out_ref):
    meta = (
        low_ref[EDGE:BLOCK, :].astype(F32)
        + own_ref[...].astype(F32)
        + high_ref[EDGE:BLOCK, :].astype(F32)
    ).astype(BF16)
    place = lax.broadcasted_iota(jnp.int32, (EXT, 256), 0)
    rho = (place % 8) * STEPS + place // 8
    spread = jnp.where(
        rho == lax.broadcasted_iota(jnp.int32, (EXT, 256), 1), jnp.float32(1), jnp.float32(0)
    ).astype(BF16)
    columns = [
        lax.dot_general(
            spread,
            meta[:, 256 * tap : 256 * tap + 256],
            (((1,), (1,)), ((), ())),
            preferred_element_type=F32,
        )
        for tap in range(TAPS)
    ]
    width = 2 * BLOCK + 128
    lane = lax.broadcasted_iota(jnp.int32, (EXT, width), 1)
    image_row = jnp.where(lane < EDGE, lane - EDGE, jnp.where(lane < BLOCK, -1000, lane - BLOCK))
    image_row = jnp.where(lane < BLOCK + 128 + EDGE, image_row, 2000)
    own_row = lax.broadcasted_iota(jnp.int32, (EXT, width), 0)
    own_row = (own_row % 8) * STEPS + own_row // 8 - HALO
    offset = (image_row - own_row + 1).astype(F32) - columns[0][:, 3:4]
    value = jnp.zeros((EXT, width), F32)
    for tap in range(TAPS):
        weight = columns[tap][:, 0:1] + columns[tap][:, 1:2] + columns[tap][:, 2:3]
        value = jnp.where(offset == float(tap), weight, value)
    hi, mid, lo = split3(value)
    source = jnp.concatenate([low_ref[...], img_ref[...], high_ref[...]], axis=0)
    total = jnp.zeros((EXT, 1024), F32)
    for piece in (lo, mid, hi):
        total = total + jnp.dot(piece.astype(BF16), source, preferred_element_type=F32)
    row_warped = total.astype(BF16)
    for pair in range(TILES // 2):
        cols = jnp.dot(
            row_warped, matrix_ref[:, 256 * pair : 256 * pair + 256], preferred_element_type=F32
        ).astype(BF16)
        out_ref[2 * pair] = cols[:, :128]
        out_ref[2 * pair + 1] = cols[:, 128:]


def row_bounds(strip):
    first = jnp.where(strip == 0, HALO, 0)
    last = jnp.where(strip == 15, HALO + 128, EXT)
    return first, last


def own_stats(x_ref, x_wide, sum_x, root_x, box_a, box_b):
    def rows(m, carry):
        value = x_ref[m].astype(F32)
        x_wide[m] = value
        put_rows(box_a, m, row_window(steps_of(value)))
        put_rows(box_b, m, row_window(steps_of(value * value)))
        return carry

    lax.fori_loop(0, TILES, rows, 0)
    edges = lanes()

    def cols(k, carry):
        at = pl.multiple_of(8 * k, 8)
        s1 = col_window(get_tiles(box_a, at), *edges)
        s2 = col_window(get_tiles(box_b, at), *edges)
        for m in range(TILES):
            sum_x[m, pl.ds(at, 8), :] = s1[m]
            root_x[m, pl.ds(at, 8), :] = lax.rsqrt(
                s2[m] - s1[m] * s1[m] * (1.0 / CELLS) + 0.25 * CELLS
            )
        return carry

    lax.fori_loop(0, STEPS, cols, 0)


def add_pair(y_ref, weight, bounds, first, x_wide, sum_x, root_x, sum_g, sum_h, sum_t, y_wide, coef, box_a, box_b, box_c):
    def rows(m, carry):
        value = y_ref[m].astype(F32)
        y_wide[m] = value
        put_rows(box_a, m, row_window(steps_of(value)))
        put_rows(box_b, m, row_window(steps_of(value * value)))
        put_rows(box_c, m, row_window(steps_of(value * x_wide[m])))
        return carry

    lax.fori_loop(0, TILES, rows, 0)
    edges = lanes()

    def cols(k, carry):
        at = pl.multiple_of(8 * k, 8)
        rho = lax.broadcasted_iota(jnp.int32, (8, 128), 0) * STEPS + k
        scale = jnp.where((rho >= bounds[0]) & (rho < bounds[1]), weight, jnp.float32(0))
        s1 = col_window(get_tiles(box_a, at), *edges)
        s2 = col_window(get_tiles(box_b, at), *edges)
        s3 = col_window(get_tiles(box_c, at), *edges)
        for m in range(TILES):
            here = (m, pl.ds(at, 8), slice(None))
            mean = s1[m] * (1.0 / CELLS)
            root = lax.rsqrt(s2[m] - s1[m] * mean + 0.25 * CELLS)
            cov = s3[m] - sum_x[here] * mean
            u = scale * root_x[here] * root
            coef[here] = u
            g, h = u * cov, u * s1[m]
            sum_g[here] = g if first else sum_g[here] + g
            sum_h[here] = h if first else sum_h[here] + h
        return carry

    lax.fori_loop(0, STEPS, cols, 0)

    def rows_2(m, carry):
        put_rows(box_a, m, row_window(steps_of(coef[m])))
        return carry

    lax.fori_loop(0, TILES, rows_2, 0)

    def cols_2(k, carry):
        at = pl.multiple_of(8 * k, 8)
        s1 = col_window(get_tiles(box_a, at), *edges)
        for m in range(TILES):
            here = (m, pl.ds(at, 8), slice(None))
            t = y_wide[here] * s1[m]
            sum_t[here] = t if first else sum_t[here] + t
        return carry

    lax.fori_loop(0, STEPS, cols_2, 0)


def finish(bounds, x_wide, sum_x, root_x, sum_g, sum_h, sum_t, natural, grad_ref, disp_ref, box_a, box_b, field_a, field_b):
    edges = lanes()

    def rows(m, carry):
        root = root_x[m]
        g = root * root * sum_g[m]
        put_rows(box_a, m, row_window(steps_of(sum_h[m] - g * sum_x[m])))
        put_rows(box_b, m, row_window(steps_of(g)))
        return carry

    lax.fori_loop(0, TILES, rows, 0)

    def cols(k, carry):
        at = pl.multiple_of(8 * k, 8)
        s1 = col_window(get_tiles(box_a, at), *edges)
        s2 = col_window(get_tiles(box_b, at), *edges)
        for m in range(TILES):
            here = (m, pl.ds(at, 8), slice(None))
            grad = s1[m] * (1.0 / CELLS) + x_wide[here] * s2[m] - sum_t[here]
            sum_t[here] = grad
            natural[0, pl.ds(m * EXT + k, 8, stride=STEPS), :] = grad
        return carry

    lax.fori_loop(0, STEPS, cols, 0)
    sub = lax.broadcasted_iota(jnp.int32, (8, 128), 0) * STEPS
    for m in range(TILES):
        x = steps_of(x_wide[m])
        seq = [pltpu.roll(x[-1], 1, 0)] + x + [pltpu.roll(x[0], SUBS - 1, 0)]
        out = []
        before = x_wide[m - 1] if m else None
        after = x_wide[m + 1] if m < TILES - 1 else None
        prods = []
        for k in range(STEPS):
            rho = sub + k
            inside = (rho >= bounds[0]) & (rho < bounds[1])
            grad = jnp.where(inside, sum_t[m, 8 * k : 8 * k + 8, :] * (-0.5 / 9.0), 0.0)
            out.append(grad * (seq[k + 2] - seq[k]))
            if m:
                left = before[8 * k : 8 * k + 8]
            else:
                left = jnp.where(edges[0], 0.0, pltpu.roll(x_wide[TILES - 1, 8 * k : 8 * k + 8, :], 1, 1))
            if m < TILES - 1:
                right = after[8 * k : 8 * k + 8]
            else:
                right = jnp.where(edges[1], 0.0, pltpu.roll(x_wide[0, 8 * k : 8 * k + 8, :], 127, 1))
            prods.append(grad * (right - left))
        put_rows(box_a, m, row_window(out))
        put_rows(box_b, m, row_window(prods))

    def cols_2(k, carry):
        at = pl.multiple_of(8 * k, 8)
        s1 = col_window(get_tiles(box_a, at), *edges)
        s2 = col_window(get_tiles(box_b, at), *edges)
        for m in range(TILES):
            natural[1, pl.ds(m * EXT + k, 8, stride=STEPS), :] = s1[m]
            natural[2, pl.ds(m * EXT + k, 8, stride=STEPS), :] = s2[m]
        return carry

    lax.fori_loop(0, STEPS, cols_2, 0)
    lane = lax.broadcasted_iota(jnp.int32, (8, 128), 1)
    pick = (lane % 8) * 16 + lane // 8

    def restore(block, carry):
        for field in range(3):
            v = [natural[field, pl.ds(m * EXT + HALO + 8 * block, 8), :] for m in range(TILES)]
            for bit in range(3):
                span = 16 << bit
                upper = (lane & span) != 0
                new = list(v)
                for m in range(TILES):
                    if m & (1 << bit):
                        continue
                    a, b = v[m], v[m | (1 << bit)]
                    new[m] = jnp.where(upper, pltpu.roll(b, span, 1), a)
                    new[m | (1 << bit)] = jnp.where(upper, b, pltpu.roll(a, 128 - span, 1))
                v = new
            for j in range(TILES):
                tile = jnp.take_along_axis(v[j], pick, axis=1)
                at = pl.ds(pl.multiple_of(8 * block, 8), 8)
                if field == 0:
                    grad_ref[at, 128 * j : 128 * j + 128] = tile
                else:
                    disp_ref[field - 1, at, 128 * j : 128 * j + 128] = tile
        return carry

    lax.fori_loop(0, 16, restore, 0)


def pair_weight(pair_on, own, other):
    low = jnp.minimum(own, other)
    gap = jnp.abs(own - other)
    inside = (other >= 0) & (other < 16)
    on = pair_on[jnp.clip(low, 0, 15), jnp.clip(gap - 1, 0, 2)]
    return jnp.where(inside, on, 0).astype(F32)


def others(own):
    partner = own + 1 - 2 * (own % 2)
    return {
        "a": partner,
        "b": own - 2,
        "c": own + 2,
        "d": jnp.where(own % 2 == 0, own - 3, own + 3),
        "e": partner - 2,
        "f": partner + 2,
    }


def field():
    return pltpu.VMEM((TILES, EXT, 128), F32)


def main_kernel(
    place, pair_on, x, ya, yb, yc, yd, ye, yf, grad, disp, x_wide, y_wide, sum_x, root_x, g, h, t, coef, box_a, box_b, box_c, natural
):
    own, strip = place[0], place[1]
    bounds = row_bounds(strip)
    own_stats(x, x_wide, sum_x, root_x, box_a, box_b)
    names = others(own)
    for i, (name, y) in enumerate(zip("abcdef", (ya, yb, yc, yd, ye, yf))):
        weight = pair_weight(pair_on, own, names[name])
        add_pair(y, weight, bounds, i == 0, x_wide, sum_x, root_x, g, h, t, y_wide, coef, box_a, box_b, box_c)
    finish(bounds, x_wide, sum_x, root_x, g, h, t, natural, grad, disp, box_a, box_b, box_c, coef)


def shape(dims, kind):
    return jax.ShapeDtypeStruct(dims, kind)


def exchange(value, axis, pairs):
    return lax.ppermute(value, axis, pairs)


def per_device(images, row_weights, row_shift, col_weights, col_shift, pair_on):
    place = jnp.stack([lax.axis_index("sec"), lax.axis_index("strip")]).astype(jnp.int32)
    image = images[0]
    big = pltpu.CompilerParams(vmem_limit_bytes=50 * 1024 * 1024)
    up, down, own = pl.pallas_call(
        prep_kernel,
        out_shape=(shape((BLOCK, 1024), BF16), shape((BLOCK, 1024), BF16), shape((8, 1024), BF16)),
        in_specs=[SMEM, VMEM, VMEM],
        out_specs=(VMEM, VMEM, VMEM),
        name="prep",
    )(row_shift, image, row_weights[0])
    low = exchange(up, "strip", [(i, i + 1) for i in range(15)])
    high = exchange(down, "strip", [(i + 1, i) for i in range(15)])
    taps = col_weights[0].reshape(TAPS, 128, 8).transpose(0, 2, 1).reshape(TAPS, 1024)
    matrix = pl.pallas_call(
        matrix_kernel,
        out_shape=shape((1024, 1024), BF16),
        in_specs=[SMEM, VMEM],
        out_specs=VMEM,
        name="matrix",
        cost_estimate=pl.CostEstimate(flops=2_000_000, bytes_accessed=2_000_000, transcendentals=0),
    )(col_shift, taps)
    warped = pl.pallas_call(
        warp_kernel,
        out_shape=shape((TILES, EXT, 128), BF16),
        in_specs=[VMEM] * 5,
        out_specs=VMEM,
        compiler_params=big,
        name="warp",
    )(image, low, high, own, matrix)
    sections = range(16)
    from_b = exchange(warped, "sec", [(s, s + 2) for s in sections if s + 2 < 16])
    from_c = exchange(warped, "sec", [(s, s - 2) for s in sections if s >= 2])
    odd = [(s, s + 3) if s % 2 else (s, s - 3) for s in sections]
    from_d = exchange(warped, "sec", [p for p in odd if 0 <= p[1] < 16])
    partner = [(s, s ^ 1) for s in sections]
    from_a = exchange(warped, "sec", partner)
    from_e = exchange(from_b, "sec", partner)
    from_f = exchange(from_c, "sec", partner)
    grad, disp = pl.pallas_call(
        main_kernel,
        out_shape=(shape((128, 1024), F32), shape((2, 128, 1024), F32)),
        in_specs=[SMEM, SMEM] + [VMEM] * 7,
        out_specs=(VMEM, VMEM),
        scratch_shapes=[field() for _ in range(11)] + [pltpu.VMEM((3, TILES * EXT, 128), F32)],
        compiler_params=big,
        name="pairs",
    )(place, pair_on, warped, from_a, from_b, from_c, from_d, from_e, from_f)
    return grad[None], disp[:, None]


def solution(mesh):
    return jax.shard_map(
        per_device,
        mesh=mesh,
        in_specs=(
            P("sec", "strip", None),
            P("sec", None, "strip"),
            P("sec", "strip"),
            P("sec", None, None),
            P("sec"),
            P(),
        ),
        out_specs=(P("sec", "strip", None), P(None, "sec", "strip", None)),
        check_vma=False,
    )
```

```python
import functools

import jax
import jax.numpy as jnp
from jax import lax
from jax.experimental import pallas as pl
from jax.experimental.pallas import tpu as pltpu
from jax.sharding import PartitionSpec as P

TAPS = 4
HALO = 12
STEPS = 19
SUBS = 8
EXT = STEPS * SUBS
TILES = 8
CELLS = 81.0
F32 = jnp.float32
BF16 = jnp.bfloat16
VMEM = pl.BlockSpec(memory_space=pltpu.VMEM)
SMEM = pl.BlockSpec(memory_space=pltpu.SMEM)
EDGE = 24
BLOCK = 32


def window_sums(seq, width):
    count = len(seq) - width + 1
    out = [None] * count
    for base in range(0, count, width):
        suffix = [None] * width
        suffix[width - 1] = seq[base + width - 1]
        for i in range(width - 2, -1, -1):
            suffix[i] = seq[base + i] + suffix[i + 1]
        prefix = None
        for i in range(width):
            if base + i >= count:
                break
            if i == 0:
                out[base] = suffix[0]
            else:
                nxt = seq[base + width + i - 1]
                prefix = nxt if prefix is None else prefix + nxt
                out[base + i] = suffix[i] + prefix
    return out


def row_window(steps):
    low = [pltpu.roll(v, 1, 0) for v in steps[-4:]]
    high = [pltpu.roll(v, SUBS - 1, 0) for v in steps[:4]]
    return window_sums(low + steps + high, 9)


def col_window(seq):
    suffix = [None] * 8
    suffix[7] = seq[7]
    for i in range(6, -1, -1):
        suffix[i] = seq[i] + suffix[i + 1]
    out = []
    prefix = None
    for i in range(8):
        prefix = seq[8 + i] if prefix is None else prefix + seq[8 + i]
        out.append(suffix[i] + prefix)
    return out


def steps_of(value):
    return [value[8 * k : 8 * k + 8] for k in range(STEPS)]


def put_rows(ref, tile, values):
    for k, v in enumerate(values):
        ref[tile, 8 * k : 8 * k + 8, :] = v


def over_tiles(body, each=4):
    lane = lax.broadcasted_iota(jnp.int32, (8, 128), 1)

    def half(h, carry):
        shift = jnp.where(h == 0, 127, 1)
        keep = lane != jnp.where(h == 0, 127, 0)

        def turn(v):
            return jnp.where(keep, pltpu.roll(v, shift, 1), 0.0)

        for i in range(4):
            body(4 * h + i, turn)
        return carry

    lax.fori_loop(0, 2, half, 0)


def put_box(pair, m, turn, values):
    main, side = pair
    sums = row_window(values)
    put_rows(side, m, [turn(v) for v in sums])
    put_rows(main, m, sums)


def get_box(pair, at):
    main, side = pair
    rows = pl.ds(at, 8)
    seq = [side[m, rows, :] for m in range(4, 8)]
    seq += [main[m, rows, :] for m in range(8)]
    seq += [side[m, rows, :] for m in range(4)]
    return col_window(seq)


def over_steps(body):
    def step(k, carry):
        body(k, pl.multiple_of(8 * k, 8))
        return carry

    lax.fori_loop(0, STEPS, step, 0)


def split3(value):
    hi = value.astype(BF16).astype(F32)
    rest = value - hi
    mid = rest.astype(BF16).astype(F32)
    return hi, mid, rest - mid


def exchange_stage(ref, lead, bit, blocks, first, each):
    lane = lax.broadcasted_iota(jnp.int32, (8, 128), 1)
    span = 16 << bit
    upper = (lane & span) != 0

    def step(s, carry):
        for e in range(each):
            at = pl.ds(pl.multiple_of(8 * (s * each + e), 8) + first, 8)
            for which in lead:
                for m in range(TILES):
                    if m & (1 << bit):
                        continue
                    lo, hi = which + (m, at), which + (m | (1 << bit), at)
                    a, b = ref[lo], ref[hi]
                    ref[lo] = jnp.where(upper, pltpu.roll(b, span, 1), a)
                    ref[hi] = jnp.where(upper, b, pltpu.roll(a, 128 - span, 1))
        return carry

    lax.fori_loop(0, blocks // each, step, 0)


def prep_kernel(shift_ref, img_ref, weights_ref, taps_ref, up_ref, down_ref, own_ref, img_out, taps_out, work):
    shift = jnp.full((1, 128), shift_ref[0, 0], jnp.int32).astype(F32)
    lane = lax.broadcasted_iota(jnp.int32, (8, 128), 1)
    row = lax.broadcasted_iota(jnp.int32, (8, 128), 0)
    zero = jnp.zeros((8, 128), F32)
    pick = 8 * (lane % 16) + lane // 16
    for j in range(TILES):
        cols = slice(128 * j, 128 * j + 128)
        tile = img_ref[:, cols].astype(F32)
        for b in range(16):
            work[j, 8 * b : 8 * b + 8, :] = jnp.take_along_axis(tile[8 * b : 8 * b + 8], pick, axis=1)
        taps = jnp.concatenate([taps_ref[:, cols].astype(F32), zero[:4]], axis=0)
        work[j, 128:136, :] = jnp.take_along_axis(taps, pick, axis=1)
    for bit in range(3):
        exchange_stage(work, [()], bit, 17, 0, 17)
    for m in range(TILES):
        cols = slice(128 * m, 128 * m + 128)
        tile = work[m, 0:128, :].astype(BF16)
        img_out[:, cols] = tile
        up_ref[0:EDGE, cols] = tile[128 - EDGE :]
        down_ref[0:EDGE, cols] = tile[:EDGE]
        taps_out[m] = work[m, 128:136, :]
    for tap in range(TAPS):
        line = jnp.broadcast_to(weights_ref[tap : tap + 1, :], (8, 128))
        hi, mid, lo = split3(pltpu.roll(line, HALO, 1))
        full = jnp.where(row == 0, hi, jnp.where(row == 1, mid, jnp.where(row == 2, lo, zero)))
        if tap == 0:
            full = jnp.where(row == 3, jnp.broadcast_to(shift, (8, 128)), full)
        at = 256 * tap
        wrapped = jnp.where(lane < HALO, full, zero).astype(BF16)
        own_ref[:, at : at + 128] = jnp.where(lane >= HALO, full, zero).astype(BF16)
        own_ref[:, at + 128 : at + 256] = wrapped
        up_ref[EDGE:BLOCK, at : at + 128] = wrapped
        up_ref[EDGE:BLOCK, at + 128 : at + 256] = zero.astype(BF16)
        down_ref[EDGE:BLOCK, at : at + 128] = zero.astype(BF16)
        down_ref[EDGE:BLOCK, at + 128 : at + 256] = jnp.where(
            (lane >= HALO) & (lane < 2 * HALO), full, zero
        ).astype(BF16)


def warp_kernel(shift_ref, img_ref, low_ref, high_ref, own_ref, taps_ref, out_ref, row_warped, virtual):
    meta = (
        low_ref[EDGE:BLOCK, :].astype(F32)
        + own_ref[...].astype(F32)
        + high_ref[EDGE:BLOCK, :].astype(F32)
    ).astype(BF16)
    place = lax.broadcasted_iota(jnp.int32, (EXT, 256), 0)
    rho = (place % 8) * STEPS + place // 8
    spread = jnp.where(
        rho == lax.broadcasted_iota(jnp.int32, (EXT, 256), 1), jnp.float32(1), jnp.float32(0)
    ).astype(BF16)
    columns = [
        lax.dot_general(
            spread,
            meta[:, 256 * tap : 256 * tap + 256],
            (((1,), (1,)), ((), ())),
            preferred_element_type=F32,
        )
        for tap in range(TAPS)
    ]
    width = 2 * BLOCK + 128
    lane = lax.broadcasted_iota(jnp.int32, (EXT, width), 1)
    image_row = jnp.where(lane < EDGE, lane - EDGE, jnp.where(lane < BLOCK, -1000, lane - BLOCK))
    image_row = jnp.where(lane < BLOCK + 128 + EDGE, image_row, 2000)
    own_row = lax.broadcasted_iota(jnp.int32, (EXT, width), 0)
    own_row = (own_row % 8) * STEPS + own_row // 8 - HALO
    offset = (image_row - own_row + 1).astype(F32) - columns[0][:, 3:4]
    value = jnp.zeros((EXT, width), F32)
    for tap in range(TAPS):
        weight = columns[tap][:, 0:1] + columns[tap][:, 1:2] + columns[tap][:, 2:3]
        value = jnp.where(offset == float(tap), weight, value)
    hi, mid, lo = split3(value)
    source = jnp.concatenate([low_ref[...], img_ref[...], high_ref[...]], axis=0)
    total = jnp.zeros((EXT, 1024), F32)
    for piece in (lo, mid, hi):
        total = total + jnp.dot(piece.astype(BF16), source, preferred_element_type=F32)
    rounded = total.astype(BF16).astype(F32)
    for m in range(TILES):
        row_warped[m] = rounded[:, 128 * m : 128 * m + 128]
    first = shift_ref[0] - 1
    lane = lax.broadcasted_iota(jnp.int32, (EXT, 128), 1)
    for v in range(TILES + TAPS - 1):
        column = first + v
        tile = lax.bitwise_and(column, 7)
        far = lax.shift_right_arithmetic(column, 3)
        moved = pltpu.roll(row_warped[tile], lax.bitwise_and(-far, 127), 1)
        virtual[v] = jnp.where((lane + far >= 0) & (lane + far < 128), moved, 0.0)
    for m in range(TILES):
        terms = [taps_ref[m, t : t + 1, :] * virtual[m + t] for t in range(TAPS)]
        out_ref[m] = ((terms[0] + terms[1]) + (terms[2] + terms[3])).astype(BF16)


def row_bounds(strip):
    first = jnp.where(strip == 0, HALO, 0)
    last = jnp.where(strip == 15, HALO + 128, EXT)
    return first, last


def inside_rows(k, bounds):
    rho = lax.broadcasted_iota(jnp.int32, (8, 128), 0) * STEPS + k
    return (rho >= bounds[0]) & (rho < bounds[1])


def own_stats(x_ref, bounds, x_wide, sum_x, root_x, slope_r, slope_c, boxes):
    def rows(m, turn):
        value = x_ref[m].astype(F32)
        x_wide[m] = value
        steps = steps_of(value)
        put_box(boxes[0], m, turn, steps)
        put_box(boxes[1], m, turn, steps_of(value * value))
        put_rows(boxes[2][1], m, [turn(v) for v in steps])
        seq = [pltpu.roll(steps[-1], 1, 0)] + steps + [pltpu.roll(steps[0], SUBS - 1, 0)]
        put_rows(slope_r, m, [(seq[k + 2] - seq[k]) for k in range(STEPS)])

    over_tiles(rows)

    def cols(k, at):
        s1 = get_box(boxes[0], at)
        s2 = get_box(boxes[1], at)
        scale = jnp.where(inside_rows(k, bounds), -0.5 / 9.0, 0.0)
        rows = pl.ds(at, 8)
        x = [boxes[2][1][7, rows, :]] + [x_wide[m, rows, :] for m in range(8)] + [boxes[2][1][0, rows, :]]
        for m in range(TILES):
            sum_x[m, rows, :] = s1[m]
            root_x[m, rows, :] = lax.rsqrt(s2[m] - s1[m] * s1[m] * (1.0 / CELLS) + 0.25 * CELLS)
            slope_r[m, rows, :] = slope_r[m, rows, :] * scale
            slope_c[m, rows, :] = (x[m + 2] - x[m]) * scale

    over_steps(cols)


def add_pair(y_ref, weight, bounds, first, x_wide, sum_x, root_x, sum_g, sum_h, sum_t, y_wide, coef, boxes):
    def rows(m, turn):
        value = y_ref[m].astype(F32)
        y_wide[m] = value
        put_box(boxes[0], m, turn, steps_of(value))
        put_box(boxes[1], m, turn, steps_of(value * value))
        put_box(boxes[2], m, turn, steps_of(value * x_wide[m]))

    over_tiles(rows)

    def cols(k, at):
        scale = jnp.where(inside_rows(k, bounds), weight, jnp.float32(0))
        s1 = get_box(boxes[0], at)
        s2 = get_box(boxes[1], at)
        s3 = get_box(boxes[2], at)
        for m in range(TILES):
            here = (m, pl.ds(at, 8), slice(None))
            mean = s1[m] * (1.0 / CELLS)
            root = lax.rsqrt(s2[m] - s1[m] * mean + 0.25 * CELLS)
            cov = s3[m] - sum_x[here] * mean
            u = scale * root_x[here] * root
            coef[here] = u
            g, h = u * cov, u * s1[m]
            sum_g[here] = g if first else sum_g[here] + g
            sum_h[here] = h if first else sum_h[here] + h

    over_steps(cols)

    def rows_2(m, turn):
        put_box(boxes[0], m, turn, steps_of(coef[m]))

    over_tiles(rows_2)

    def cols_2(k, at):
        s1 = get_box(boxes[0], at)
        for m in range(TILES):
            here = (m, pl.ds(at, 8), slice(None))
            t = y_wide[here] * s1[m]
            sum_t[here] = t if first else sum_t[here] + t

    over_steps(cols_2)


def finish(x_wide, sum_x, root_x, slope_r, slope_c, sum_g, sum_h, sum_t, natural, grad_ref, disp_ref, boxes):
    def rows(m, turn):
        root = root_x[m]
        g = root * root * sum_g[m]
        put_box(boxes[0], m, turn, steps_of(sum_h[m] - g * sum_x[m]))
        put_box(boxes[1], m, turn, steps_of(g))

    over_tiles(rows)

    def cols(k, at):
        s1 = get_box(boxes[0], at)
        s2 = get_box(boxes[1], at)
        for m in range(TILES):
            here = (m, pl.ds(at, 8), slice(None))
            grad = s1[m] * (1.0 / CELLS) + x_wide[here] * s2[m] - sum_t[here]
            natural[0, m, pl.ds(k, 8, stride=STEPS), :] = grad
            sum_g[here] = grad * slope_r[here]
            sum_h[here] = grad * slope_c[here]

    over_steps(cols)

    def rows_2(m, turn):
        put_box(boxes[0], m, turn, steps_of(sum_g[m]))
        put_box(boxes[1], m, turn, steps_of(sum_h[m]))

    over_tiles(rows_2)

    def cols_2(k, at):
        s1 = get_box(boxes[0], at)
        s2 = get_box(boxes[1], at)
        for m in range(TILES):
            natural[1, m, pl.ds(k, 8, stride=STEPS), :] = s1[m]
            natural[2, m, pl.ds(k, 8, stride=STEPS), :] = s2[m]

    over_steps(cols_2)
    for bit in range(3):
        exchange_stage(natural, [(0,), (1,), (2,)], bit, 16, HALO, 8)
    lane = lax.broadcasted_iota(jnp.int32, (8, 128), 1)
    pick = (lane % 8) * 16 + lane // 8

    def restore(step, carry):
        for e in range(8):
            at = pl.multiple_of(8 * (8 * step + e), 8)
            for which in range(3):
                for j in range(TILES):
                    tile = jnp.take_along_axis(natural[which, j, pl.ds(at + HALO, 8), :], pick, axis=1)
                    if which == 0:
                        grad_ref[pl.ds(at, 8), 128 * j : 128 * j + 128] = tile
                    else:
                        disp_ref[which - 1, pl.ds(at, 8), 128 * j : 128 * j + 128] = tile
        return carry

    lax.fori_loop(0, 2, restore, 0)


def pair_weight(pair_on, own, other):
    low = jnp.minimum(own, other)
    gap = jnp.abs(own - other)
    inside = (other >= 0) & (other < 16)
    on = pair_on[jnp.clip(low, 0, 15), jnp.clip(gap - 1, 0, 2)]
    return jnp.where(inside, on, 0).astype(F32)


def others(own):
    way = 1 - 2 * (own % 2)
    return [own + way, own + 2 * way, own - way, own - 2 * way, own - 3 * way, own + 3 * way]


def field():
    return pltpu.VMEM((TILES, EXT, 128), F32)


def shape(dims, kind):
    return jax.ShapeDtypeStruct(dims, kind)


FIELD = shape((TILES, EXT, 128), F32)


def own_kernel(place, x, x_wide, sum_x, root_x, slope_r, slope_c, *boxes):
    own_stats(x, row_bounds(place[1]), x_wide, sum_x, root_x, slope_r, slope_c, paired(boxes))


def paired(refs):
    return [(refs[2 * i], refs[2 * i + 1]) for i in range(3)]


def pair_kernel(turns, place, pair_on, *refs):
    ys, refs = refs[: len(turns)], refs[len(turns) :]
    first = 0 in turns
    kept = 0 if first else 3
    x_wide, sum_x, root_x = refs[:3]
    g, h, t = refs[3 + kept : 6 + kept]
    y_wide, coef = refs[6 + kept : 8 + kept]
    boxes = paired(refs[8 + kept :])
    names = others(place[0])
    for i, y in zip(turns, ys):
        weight = pair_weight(pair_on, place[0], names[i])
        add_pair(y, weight, row_bounds(place[1]), i == 0, x_wide, sum_x, root_x, g, h, t, y_wide, coef, boxes)


def last_kernel(turns, place, pair_on, *refs):
    ys, refs = refs[: len(turns)], refs[len(turns) :]
    x_wide, sum_x, root_x, slope_r, slope_c, g_in, h_in, t_in, grad, disp, g, h, t, y_wide, coef, natural = refs[:16]
    boxes = paired(refs[16:])
    names = others(place[0])
    for i, y in zip(turns, ys):
        weight = pair_weight(pair_on, place[0], names[i])
        add_pair(y, weight, row_bounds(place[1]), False, x_wide, sum_x, root_x, g, h, t, y_wide, coef, boxes)
    finish(x_wide, sum_x, root_x, slope_r, slope_c, g, h, t, natural, grad, disp, boxes)


def params(mib=24):
    return pltpu.CompilerParams(vmem_limit_bytes=mib * 1024 * 1024)


def cost(us):
    return pl.CostEstimate(flops=int(us * 4_000_000), bytes_accessed=1_000_000, transcendentals=0)


def add_pairs(turns, place, pair_on, ys, stats, sums):
    ins = [place, pair_on, *ys, *stats, *sums]
    start = len(ins) - len(sums)
    return pl.pallas_call(
        functools.partial(pair_kernel, turns),
        out_shape=(FIELD,) * 3,
        in_specs=[SMEM, SMEM] + [VMEM] * (len(ins) - 2),
        out_specs=(VMEM,) * 3,
        scratch_shapes=[field() for _ in range(8)],
        input_output_aliases={start + i: i for i in range(len(sums))},
        compiler_params=params(),
        cost_estimate=cost(1.5 * len(turns)),
        name="pair",
    )(*ins)


def per_device(images, row_weights, row_shift, col_weights, col_shift, pair_on):
    place = jnp.stack([lax.axis_index("sec"), lax.axis_index("strip")]).astype(jnp.int32)
    block = shape((BLOCK, 1024), BF16)
    up, down, own, image, taps = pl.pallas_call(
        prep_kernel,
        out_shape=(block, block, shape((8, 1024), BF16), shape((128, 1024), BF16), shape((TILES, 8, 128), F32)),
        in_specs=[SMEM, VMEM, VMEM, VMEM],
        out_specs=(VMEM,) * 5,
        scratch_shapes=[pltpu.VMEM((TILES, 136, 128), F32)],
        compiler_params=params(),
        name="prep",
    )(row_shift, images[0], row_weights[0], col_weights[0])
    low = lax.ppermute(up, "strip", [(i, i + 1) for i in range(15)])
    high = lax.ppermute(down, "strip", [(i + 1, i) for i in range(15)])
    warped = pl.pallas_call(
        warp_kernel,
        out_shape=shape((TILES, EXT, 128), BF16),
        in_specs=[SMEM] + [VMEM] * 5,
        out_specs=VMEM,
        scratch_shapes=[field(), pltpu.VMEM((TILES + TAPS - 1, EXT, 128), F32)],
        compiler_params=params(),
        name="warp",
    )(col_shift, image, low, high, own, taps)
    sections = range(16)

    def send(value, target):
        pairs = [(s, target(s, 1 - 2 * (s % 2))) for s in sections]
        return lax.ppermute(value, "sec", [p for p in pairs if 0 <= p[1] < 16])

    from_0 = send(warped, lambda s, way: s + way)
    from_1 = send(warped, lambda s, way: s - 2 * way)
    from_2 = send(from_1, lambda s, way: s + way)
    from_3 = send(warped, lambda s, way: s + 2 * way)
    from_4 = send(from_1, lambda s, way: s - way)
    from_5 = send(from_3, lambda s, way: s + way)
    x_wide, sum_x, root_x, slope_r, slope_c = pl.pallas_call(
        own_kernel,
        out_shape=(FIELD,) * 5,
        in_specs=[SMEM, VMEM],
        out_specs=(VMEM,) * 5,
        scratch_shapes=[field() for _ in range(6)],
        compiler_params=params(),
        cost_estimate=cost(1.3),
        name="own",
    )(place, warped)
    stats = (x_wide, sum_x, root_x)
    sums = add_pairs((0,), place, pair_on, (from_0,), stats, ())
    sums = add_pairs((1, 2), place, pair_on, (from_1, from_2), stats, sums)
    sums = add_pairs((3,), place, pair_on, (from_3,), stats, sums)
    grad, disp = pl.pallas_call(
        functools.partial(last_kernel, (4, 5)),
        out_shape=(shape((128, 1024), F32), shape((2, 128, 1024), F32)) + (FIELD,) * 3,
        in_specs=[SMEM, SMEM] + [VMEM] * 10,
        out_specs=(VMEM,) * 5,
        scratch_shapes=[field(), field(), pltpu.VMEM((3, TILES, EXT, 128), F32)] + [field() for _ in range(6)],
        input_output_aliases={9: 2, 10: 3, 11: 4},
        compiler_params=params(),
        cost_estimate=cost(5),
        name="last",
    )(place, pair_on, from_4, from_5, *stats, slope_r, slope_c, *sums)[:2]
    return grad[None], disp[:, None]


def solution(mesh):
    return jax.shard_map(
        per_device,
        mesh=mesh,
        in_specs=(
            P("sec", "strip", None),
            P("sec", None, "strip"),
            P("sec", "strip"),
            P("sec", None, None),
            P("sec"),
            P(),
        ),
        out_specs=(P("sec", "strip", None), P(None, "sec", "strip", None)),
        check_vma=False,
    )
```

```python
import functools

import jax
import jax.numpy as jnp
from jax import lax
from jax.experimental import pallas as pl
from jax.experimental.pallas import tpu as pltpu
from jax.sharding import PartitionSpec as P


TAPS = 4
HALO = 12
STEPS = 19
SUBS = 8
EXT = STEPS * SUBS
TILES = 8
CELLS = 81.0
F32 = jnp.float32
BF16 = jnp.bfloat16
VMEM = pl.BlockSpec(memory_space=pltpu.VMEM)
SMEM = pl.BlockSpec(memory_space=pltpu.SMEM)
HBM = pl.BlockSpec(memory_space=pl.ANY)
EDGE = 24
UNROLL = 3
GROUP = 8
EACH = 16
BLOCK = 32


def window_sums(seq, width):
    count = len(seq) - width + 1
    out = [None] * count
    for base in range(0, count, width):
        suffix = [None] * width
        suffix[width - 1] = seq[base + width - 1]
        for i in range(width - 2, -1, -1):
            suffix[i] = seq[base + i] + suffix[i + 1]
        prefix = None
        for i in range(width):
            if base + i >= count:
                break
            if i == 0:
                out[base] = suffix[0]
            else:
                nxt = seq[base + width + i - 1]
                prefix = nxt if prefix is None else prefix + nxt
                out[base + i] = suffix[i] + prefix
    return out


def row_window(steps):
    low = [pltpu.roll(v, 1, 0) for v in steps[-4:]]
    high = [pltpu.roll(v, SUBS - 1, 0) for v in steps[:4]]
    return window_sums(low + steps + high, 9)


def col_window(seq):
    suffix = [None] * 8
    suffix[7] = seq[7]
    for i in range(6, -1, -1):
        suffix[i] = seq[i] + suffix[i + 1]
    out = []
    prefix = None
    for i in range(8):
        prefix = seq[8 + i] if prefix is None else prefix + seq[8 + i]
        out.append(suffix[i] + prefix)
    return out


def steps_of(value):
    return [value[8 * k : 8 * k + 8] for k in range(STEPS)]


def put_rows(ref, tile, values):
    for k, v in enumerate(values):
        ref[tile, 8 * k : 8 * k + 8, :] = v


def over_tiles(body, each=GROUP):
    lane = lax.broadcasted_iota(jnp.int32, (8, 128), 1)

    def turn_to(shift, edge):
        keep = lane != edge
        return lambda v: jnp.where(keep, pltpu.roll(v, shift, 1), 0.0)

    if each == TILES:
        for m in range(TILES):
            body(m, turn_to(127, 127) if m < 4 else turn_to(1, 0))
        return

    def part(q, carry):
        low = each * q < 4
        turn = turn_to(jnp.where(low, 127, 1), jnp.where(low, 127, 0))
        for i in range(each):
            body(each * q + i, turn)
        return carry

    lax.fori_loop(0, TILES // each, part, 0)


def put_box(pair, m, turn, values):
    main, side = pair
    sums = row_window(values)
    put_rows(side, m, [turn(v) for v in sums])
    put_rows(main, m, sums)


def get_box(pair, at):
    main, side = pair
    rows = pl.ds(at, 8)
    seq = [side[m, rows, :] for m in range(4, 8)]
    seq += [main[m, rows, :] for m in range(8)]
    seq += [side[m, rows, :] for m in range(4)]
    return col_window(seq)


def over_steps(body, each=UNROLL):
    def step(i, carry):
        for e in range(each):
            k = each * i + e
            body(k, pl.multiple_of(8 * k, 8))
        return carry

    lax.fori_loop(0, STEPS // each, step, 0)
    for k in range(STEPS // each * each, STEPS):
        body(k, 8 * k)


def split3(value):
    hi = value.astype(BF16).astype(F32)
    rest = value - hi
    mid = rest.astype(BF16).astype(F32)
    return hi, mid, rest - mid


def exchange_stage(source, target, lead, bit, blocks, first, each):
    lane = lax.broadcasted_iota(jnp.int32, (8, 128), 1)
    span = 16 << bit
    upper = (lane & span) != 0

    def step(s, carry):
        for e in range(each):
            at = pl.ds(pl.multiple_of(8 * (s * each + e), 8) + first, 8)
            for which in lead:
                for m in range(TILES):
                    if m & (1 << bit):
                        continue
                    lo, hi = which + (m, at), which + (m | (1 << bit), at)
                    a, b = source[lo], source[hi]
                    target[lo] = jnp.where(upper, pltpu.roll(b, span, 1), a)
                    target[hi] = jnp.where(upper, b, pltpu.roll(a, 128 - span, 1))
        return carry

    lax.fori_loop(0, blocks // each, step, 0)


def prep_kernel(img_ref, small_ref, up_ref, down_ref, own_ref, img_out, taps_out, work, other):
    shift = small_ref[8:9, 0:128]
    lane = lax.broadcasted_iota(jnp.int32, (8, 128), 1)
    row = lax.broadcasted_iota(jnp.int32, (8, 128), 0)
    zero = jnp.zeros((8, 128), F32)
    pick = 8 * (lane % 16) + lane // 16
    for j in range(TILES):
        cols = slice(128 * j, 128 * j + 128)
        tile = img_ref[:, cols].astype(F32)
        for b in range(16):
            work[j, 8 * b : 8 * b + 8, :] = jnp.take_along_axis(tile[8 * b : 8 * b + 8], pick, axis=1)
        work[j, 128:136, :] = jnp.take_along_axis(small_ref[0:8, cols], pick, axis=1)
    exchange_stage(work, other, [()], 0, 17, 0, 17)
    exchange_stage(other, work, [()], 1, 17, 0, 17)
    exchange_stage(work, other, [()], 2, 17, 0, 17)
    for m in range(TILES):
        cols = slice(128 * m, 128 * m + 128)
        tile = other[m, 0:128, :].astype(BF16)
        img_out[:, cols] = tile
        up_ref[0:EDGE, cols] = tile[128 - EDGE :]
        down_ref[0:EDGE, cols] = tile[:EDGE]
        taps_out[m] = other[m, 128:136, :]
    for tap in range(TAPS):
        line = jnp.broadcast_to(small_ref[4 + tap : 5 + tap, 0:128], (8, 128))
        hi, mid, lo = split3(pltpu.roll(line, HALO, 1))
        full = jnp.where(row == 0, hi, jnp.where(row == 1, mid, jnp.where(row == 2, lo, zero)))
        if tap == 0:
            full = jnp.where(row == 3, jnp.broadcast_to(shift, (8, 128)), full)
        at = 256 * tap
        wrapped = jnp.where(lane < HALO, full, zero).astype(BF16)
        own_ref[:, at : at + 128] = jnp.where(lane >= HALO, full, zero).astype(BF16)
        own_ref[:, at + 128 : at + 256] = wrapped
        up_ref[EDGE:BLOCK, at : at + 128] = wrapped
        up_ref[EDGE:BLOCK, at + 128 : at + 256] = zero.astype(BF16)
        down_ref[EDGE:BLOCK, at : at + 128] = zero.astype(BF16)
        down_ref[EDGE:BLOCK, at + 128 : at + 256] = jnp.where(
            (lane >= HALO) & (lane < 2 * HALO), full, zero
        ).astype(BF16)


def warp_kernel(shift_ref, img_ref, low_ref, high_ref, own_ref, taps_ref, out_ref, row_warped, virtual):
    meta = (
        low_ref[EDGE:BLOCK, :].astype(F32)
        + own_ref[...].astype(F32)
        + high_ref[EDGE:BLOCK, :].astype(F32)
    ).astype(BF16)
    place = lax.broadcasted_iota(jnp.int32, (EXT, 256), 0)
    rho = (place % 8) * STEPS + place // 8
    spread = jnp.where(
        rho == lax.broadcasted_iota(jnp.int32, (EXT, 256), 1), jnp.float32(1), jnp.float32(0)
    ).astype(BF16)
    columns = [
        lax.dot_general(
            spread,
            meta[:, 256 * tap : 256 * tap + 256],
            (((1,), (1,)), ((), ())),
            preferred_element_type=F32,
        )
        for tap in range(TAPS)
    ]
    width = 2 * BLOCK + 128
    lane = lax.broadcasted_iota(jnp.int32, (EXT, width), 1)
    image_row = jnp.where(lane < EDGE, lane - EDGE, jnp.where(lane < BLOCK, -1000, lane - BLOCK))
    image_row = jnp.where(lane < BLOCK + 128 + EDGE, image_row, 2000)
    own_row = lax.broadcasted_iota(jnp.int32, (EXT, width), 0)
    own_row = (own_row % 8) * STEPS + own_row // 8 - HALO
    offset = (image_row - own_row + 1).astype(F32) - columns[0][:, 3:4]
    value = jnp.zeros((EXT, width), F32)
    for tap in range(TAPS):
        weight = columns[tap][:, 0:1] + columns[tap][:, 1:2] + columns[tap][:, 2:3]
        value = jnp.where(offset == float(tap), weight, value)
    hi, mid, lo = split3(value)
    source = jnp.concatenate([low_ref[...], img_ref[...], high_ref[...]], axis=0)
    total = jnp.zeros((EXT, 1024), F32)
    for piece in (lo, mid, hi):
        total = total + jnp.dot(piece.astype(BF16), source, preferred_element_type=F32)
    rounded = total.astype(BF16).astype(F32)
    for m in range(TILES):
        row_warped[m] = rounded[:, 128 * m : 128 * m + 128]
    first = shift_ref[0] - 1
    lane = lax.broadcasted_iota(jnp.int32, (EXT, 128), 1)
    for v in range(TILES + TAPS - 1):
        column = first + v
        tile = lax.bitwise_and(column, 7)
        far = lax.shift_right_arithmetic(column, 3)
        moved = pltpu.roll(row_warped[tile], lax.bitwise_and(-far, 127), 1)
        virtual[v] = jnp.where((lane + far >= 0) & (lane + far < 128), moved, 0.0)
    for m in range(TILES):
        terms = [taps_ref[m, t : t + 1, :] * virtual[m + t] for t in range(TAPS)]
        out_ref[m] = ((terms[0] + terms[1]) + (terms[2] + terms[3])).astype(BF16)


def inside_rows(k, plan):
    rho = (lax.broadcasted_iota(jnp.int32, (8, 128), 0) * STEPS + k).astype(F32)
    return (rho >= plan[6:7, :]) & (rho < plan[7:8, :])


def own_stats(x_ref, plan, x_wide, sum_x, root_x, slope_r, slope_c, boxes):
    def rows(m, turn):
        value = x_ref[m].astype(F32)
        x_wide[m] = value
        steps = steps_of(value)
        put_box(boxes[0], m, turn, steps)
        put_box(boxes[1], m, turn, steps_of(value * value))
        put_rows(boxes[2][1], m, [turn(v) for v in steps])
        seq = [pltpu.roll(steps[-1], 1, 0)] + steps + [pltpu.roll(steps[0], SUBS - 1, 0)]
        put_rows(slope_r, m, [(seq[k + 2] - seq[k]) for k in range(STEPS)])

    over_tiles(rows)

    def cols(k, at):
        s1 = get_box(boxes[0], at)
        s2 = get_box(boxes[1], at)
        scale = jnp.where(inside_rows(k, plan), -0.5 / 9.0, 0.0)
        rows = pl.ds(at, 8)
        x = [boxes[2][1][7, rows, :]] + [x_wide[m, rows, :] for m in range(8)] + [boxes[2][1][0, rows, :]]
        for m in range(TILES):
            sum_x[m, rows, :] = s1[m]
            root_x[m, rows, :] = lax.rsqrt(s2[m] - s1[m] * s1[m] * (1.0 / CELLS) + 0.25 * CELLS)
            slope_r[m, rows, :] = slope_r[m, rows, :] * scale
            slope_c[m, rows, :] = (x[m + 2] - x[m]) * scale

    over_steps(cols)


def add_pair(y_ref, which, plan, first, x_wide, sum_x, root_x, sum_g, sum_h, sum_t, y_wide, coef, boxes):
    def rows(m, turn):
        value = y_ref[m].astype(F32)
        y_wide[m] = value
        put_box(boxes[0], m, turn, steps_of(value))
        put_box(boxes[1], m, turn, steps_of(value * value))
        put_box(boxes[2], m, turn, steps_of(value * x_wide[m]))

    over_tiles(rows)

    def cols(k, at):
        scale = jnp.where(inside_rows(k, plan), plan[which : which + 1, :], 0.0)
        s1 = get_box(boxes[0], at)
        s2 = get_box(boxes[1], at)
        s3 = get_box(boxes[2], at)
        for m in range(TILES):
            here = (m, pl.ds(at, 8), slice(None))
            mean = s1[m] * (1.0 / CELLS)
            root = lax.rsqrt(s2[m] - s1[m] * mean + 0.25 * CELLS)
            cov = s3[m] - sum_x[here] * mean
            u = scale * root_x[here] * root
            coef[here] = u
            g, h = u * cov, u * s1[m]
            sum_g[here] = g if first else sum_g[here] + g
            sum_h[here] = h if first else sum_h[here] + h

    over_steps(cols)

    def rows_2(m, turn):
        put_box(boxes[0], m, turn, steps_of(coef[m]))

    over_tiles(rows_2)

    def cols_2(k, at):
        s1 = get_box(boxes[0], at)
        for m in range(TILES):
            here = (m, pl.ds(at, 8), slice(None))
            t = y_wide[here] * s1[m]
            sum_t[here] = t if first else sum_t[here] + t

    over_steps(cols_2)


def restore(natural, other, which, target):
    lead = [(w,) for w in which]
    exchange_stage(natural, other, lead, 0, 16, HALO, EACH // len(which))
    exchange_stage(other, natural, lead, 1, 16, HALO, EACH // len(which))
    exchange_stage(natural, other, lead, 2, 16, HALO, EACH // len(which))
    lane = lax.broadcasted_iota(jnp.int32, (8, 128), 1)
    pick = (lane % 8) * 16 + lane // 8
    each = EACH // len(which)

    def step(s, carry):
        for e in range(each):
            at = pl.multiple_of(8 * (each * s + e), 8)
            for w in which:
                for j in range(TILES):
                    tile = jnp.take_along_axis(other[w, j, pl.ds(at + HALO, 8), :], pick, axis=1)
                    target[w, pl.ds(at, 8), 128 * j : 128 * j + 128] = tile
        return carry

    lax.fori_loop(0, 16 // each, step, 0)


def finish(x_wide, sum_x, root_x, slope_r, slope_c, sum_g, sum_h, sum_t, natural, other, wide, sems, grad_hbm, disp_hbm, boxes):
    def rows(m, turn):
        root = root_x[m]
        g = root * root * sum_g[m]
        put_box(boxes[0], m, turn, steps_of(sum_h[m] - g * sum_x[m]))
        put_box(boxes[1], m, turn, steps_of(g))

    over_tiles(rows)

    def cols(k, at):
        s1 = get_box(boxes[0], at)
        s2 = get_box(boxes[1], at)
        for m in range(TILES):
            here = (m, pl.ds(at, 8), slice(None))
            grad = s1[m] * (1.0 / CELLS) + x_wide[here] * s2[m] - sum_t[here]
            natural[0, m, pl.ds(k, 8, stride=STEPS), :] = grad
            sum_g[here] = grad * slope_r[here]
            sum_h[here] = grad * slope_c[here]

    over_steps(cols)
    restore(natural, other, [0], wide)
    out = pltpu.make_async_copy(wide.at[0], grad_hbm, sems.at[0])
    out.start()

    def rows_2(m, turn):
        put_box(boxes[0], m, turn, steps_of(sum_g[m]))
        put_box(boxes[1], m, turn, steps_of(sum_h[m]))

    over_tiles(rows_2)

    def cols_2(k, at):
        s1 = get_box(boxes[0], at)
        s2 = get_box(boxes[1], at)
        for m in range(TILES):
            natural[1, m, pl.ds(k, 8, stride=STEPS), :] = s1[m]
            natural[2, m, pl.ds(k, 8, stride=STEPS), :] = s2[m]

    over_steps(cols_2)
    restore(natural, other, [1, 2], wide)
    out_2 = pltpu.make_async_copy(wide.at[pl.ds(1, 2)], disp_hbm, sems.at[1])
    out_2.start()
    out.wait()
    out_2.wait()


def others(own):
    way = 1 - 2 * (own % 2)
    return [own + way, own + 2 * way, own - way, own - 2 * way, own - 3 * way, own + 3 * way]


def field():
    return pltpu.VMEM((TILES, EXT, 128), F32)


def shape(dims, kind):
    return jax.ShapeDtypeStruct(dims, kind)


FIELD = shape((TILES, EXT, 128), F32)


def own_kernel(small, x, x_wide, sum_x, root_x, slope_r, slope_c, plan, *boxes):
    own, strip = lax.axis_index("sec"), lax.axis_index("strip")
    row = lax.broadcasted_iota(jnp.int32, (8, 128), 0)
    lane = lax.broadcasted_iota(jnp.int32, (8, 128), 1)
    table = small[8:16, 0:128]
    lines = jnp.where(row == 6, jnp.where(strip == 0, HALO, 0), jnp.where(strip == 15, HALO + 128, EXT)).astype(F32)
    for i, section in enumerate(others(own)):
        low, gap = jnp.minimum(own, section), jnp.abs(own - section)
        here = (row == gap) & (lane == low) & (section >= 0) & (section < 16)
        weight = jnp.sum(jnp.sum(jnp.where(here, table, 0.0), axis=1, keepdims=True), axis=0, keepdims=True)
        lines = jnp.where(row == i, weight, lines)
    plan[...] = lines
    own_stats(x, lines, x_wide, sum_x, root_x, slope_r, slope_c, paired(boxes))


def paired(refs):
    return [(refs[2 * i], refs[2 * i + 1]) for i in range(3)]


def pair_kernel(turns, plan, *refs):
    ys, refs = refs[: len(turns)], refs[len(turns) :]
    first = 0 in turns
    kept = 0 if first else 3
    x_wide, sum_x, root_x = refs[:3]
    g, h, t = refs[3 + kept : 6 + kept]
    y_wide, coef = refs[6 + kept : 8 + kept]
    boxes = paired(refs[8 + kept :])
    for i, y in zip(turns, ys):
        add_pair(y, i, plan[...], i == 0, x_wide, sum_x, root_x, g, h, t, y_wide, coef, boxes)


def last_kernel(turns, plan, *refs):
    ys, refs = refs[: len(turns)], refs[len(turns) :]
    x_wide, sum_x, root_x, slope_r, slope_c, _, _, _, grad, disp, g, h, t, y_wide, coef, natural, other, wide, sems = refs[:19]
    boxes = paired(refs[19:])
    for i, y in zip(turns, ys):
        add_pair(y, i, plan[...], False, x_wide, sum_x, root_x, g, h, t, y_wide, coef, boxes)
    finish(x_wide, sum_x, root_x, slope_r, slope_c, g, h, t, natural, other, wide, sems, grad, disp, boxes)


def last_scratch():
    three = pltpu.VMEM((3, TILES, EXT, 128), F32)
    wide = pltpu.VMEM((3, 128, 1024), F32)
    return [field(), field(), three, three, wide, pltpu.SemaphoreType.DMA((2,))] + [field() for _ in range(6)]


def params(mib=24):
    return pltpu.CompilerParams(vmem_limit_bytes=mib * 1024 * 1024)


def cost(us):
    return pl.CostEstimate(flops=int(us * 4_000_000), bytes_accessed=1_000_000, transcendentals=0)


def add_pairs(turns, plan, ys, stats, sums):
    ins = [plan, *ys, *stats, *sums]
    start = len(ins) - len(sums)
    return pl.pallas_call(
        functools.partial(pair_kernel, turns),
        out_shape=(FIELD,) * 3,
        in_specs=[VMEM] * len(ins),
        out_specs=(VMEM,) * 3,
        scratch_shapes=[field() for _ in range(8)],
        input_output_aliases={start + i: i for i in range(len(sums))},
        compiler_params=params(),
        cost_estimate=cost(1.5 * len(turns)),
        name="pair",
    )(*ins)


def per_device(images, row_weights, row_shift, col_weights, col_shift, pair_on):
    block = shape((BLOCK, 1024), BF16)

    def wide(value):
        return jnp.pad(value.astype(F32), ((0, 0), (0, 1024 - value.shape[1])))

    small = jnp.concatenate(
        [
            col_weights[0].astype(F32),
            wide(row_weights[0]),
            jnp.broadcast_to(row_shift.astype(F32), (1, 1024)),
            wide(pair_on.T),
            jnp.zeros((4, 1024), F32),
        ]
    )
    up, down, own, image, taps = pl.pallas_call(
        prep_kernel,
        out_shape=(
            block,
            block,
            shape((8, 1024), BF16),
            shape((128, 1024), BF16),
            shape((TILES, 8, 128), F32),
        ),
        in_specs=[VMEM] * 2,
        out_specs=(VMEM,) * 5,
        scratch_shapes=[pltpu.VMEM((TILES, 136, 128), F32)] * 2,
        compiler_params=params(),
        name="prep",
    )(images[0], small)
    low = lax.ppermute(up, "strip", [(i, i + 1) for i in range(15)])
    high = lax.ppermute(down, "strip", [(i + 1, i) for i in range(15)])
    warped = pl.pallas_call(
        warp_kernel,
        out_shape=shape((TILES, EXT, 128), BF16),
        in_specs=[SMEM] + [VMEM] * 5,
        out_specs=VMEM,
        scratch_shapes=[field(), pltpu.VMEM((TILES + TAPS - 1, EXT, 128), F32)],
        compiler_params=params(),
        name="warp",
    )(col_shift, image, low, high, own, taps)
    sections = range(16)

    def send(value, target):
        pairs = [(s, target(s, 1 - 2 * (s % 2))) for s in sections]
        return lax.ppermute(value, "sec", [p for p in pairs if 0 <= p[1] < 16])

    from_0 = send(warped, lambda s, way: s + way)
    from_1 = send(warped, lambda s, way: s - 2 * way)
    from_2 = send(from_1, lambda s, way: s + way)
    from_3 = send(warped, lambda s, way: s + 2 * way)
    from_4 = send(from_1, lambda s, way: s - way)
    from_5 = send(from_3, lambda s, way: s + way)
    x_wide, sum_x, root_x, slope_r, slope_c, plan = pl.pallas_call(
        own_kernel,
        out_shape=(FIELD,) * 5 + (shape((8, 128), F32),),
        in_specs=[VMEM, VMEM],
        out_specs=(VMEM,) * 6,
        scratch_shapes=[field() for _ in range(6)],
        compiler_params=params(),
        cost_estimate=cost(1.3),
        name="own",
    )(small, warped)
    stats = (x_wide, sum_x, root_x)
    sums = ()
    for i, y in enumerate((from_0, from_1, from_2, from_3, from_4)):
        sums = add_pairs((i,), plan, (y,), stats, sums)
    grad, disp = pl.pallas_call(
        functools.partial(last_kernel, (5,)),
        out_shape=(shape((128, 1024), F32), shape((2, 128, 1024), F32)) + (FIELD,) * 3,
        in_specs=[VMEM] * 10,
        out_specs=(HBM, HBM) + (VMEM,) * 3,
        scratch_shapes=last_scratch(),
        input_output_aliases={7: 2, 8: 3, 9: 4},
        compiler_params=params(),
        cost_estimate=cost(5),
        name="last",
    )(plan, from_5, *stats, slope_r, slope_c, *sums)[:2]
    return grad[None], disp[:, None]


def solution(mesh):
    return jax.shard_map(
        per_device,
        mesh=mesh,
        in_specs=(
            P("sec", "strip", None),
            P("sec", None, "strip"),
            P("sec", "strip"),
            P("sec", None, None),
            P("sec"),
            P(),
        ),
        out_specs=(P("sec", "strip", None), P(None, "sec", "strip", None)),
        check_vma=False,
    )
```

```python
import functools

import jax
import jax.numpy as jnp
from jax import lax
from jax.experimental import pallas as pl
from jax.experimental.pallas import tpu as pltpu
from jax.sharding import PartitionSpec as P


TAPS = 4
HALO = 12
STEPS = 19
SUBS = 8
EXT = STEPS * SUBS
TILES = 8
CELLS = 81.0
F32 = jnp.float32
BF16 = jnp.bfloat16
VMEM = pl.BlockSpec(memory_space=pltpu.VMEM)
SMEM = pl.BlockSpec(memory_space=pltpu.SMEM)
HBM = pl.BlockSpec(memory_space=pl.ANY)
EDGE = 24
UNROLL = 3
GROUP = 8
EACH = 16
BLOCK = 32


def window_sums(seq, width):
    count = len(seq) - width + 1
    out = [None] * count
    for base in range(0, count, width):
        suffix = [None] * width
        suffix[width - 1] = seq[base + width - 1]
        for i in range(width - 2, -1, -1):
            suffix[i] = seq[base + i] + suffix[i + 1]
        prefix = None
        for i in range(width):
            if base + i >= count:
                break
            if i == 0:
                out[base] = suffix[0]
            else:
                nxt = seq[base + width + i - 1]
                prefix = nxt if prefix is None else prefix + nxt
                out[base + i] = suffix[i] + prefix
    return out


def row_window(steps):
    low = [pltpu.roll(v, 1, 0) for v in steps[-4:]]
    high = [pltpu.roll(v, SUBS - 1, 0) for v in steps[:4]]
    return window_sums(low + steps + high, 9)


def col_window(seq):
    suffix = [None] * 8
    suffix[7] = seq[7]
    for i in range(6, -1, -1):
        suffix[i] = seq[i] + suffix[i + 1]
    out = []
    prefix = None
    for i in range(8):
        prefix = seq[8 + i] if prefix is None else prefix + seq[8 + i]
        out.append(suffix[i] + prefix)
    return out


def steps_of(value):
    return [value[8 * k : 8 * k + 8] for k in range(STEPS)]


def put_rows(ref, tile, values):
    for k, v in enumerate(values):
        ref[tile, 8 * k : 8 * k + 8, :] = v


def over_tiles(body, each=GROUP):
    lane = lax.broadcasted_iota(jnp.int32, (8, 128), 1)

    def turn_to(shift, edge):
        keep = lane != edge
        return lambda v: jnp.where(keep, pltpu.roll(v, shift, 1), 0.0)

    if each == TILES:
        for m in range(TILES):
            body(m, turn_to(127, 127) if m < 4 else turn_to(1, 0))
        return

    def part(q, carry):
        low = each * q < 4
        turn = turn_to(jnp.where(low, 127, 1), jnp.where(low, 127, 0))
        for i in range(each):
            body(each * q + i, turn)
        return carry

    lax.fori_loop(0, TILES // each, part, 0)


def put_box(pair, m, turn, values):
    main, side = pair
    sums = row_window(values)
    put_rows(side, m, [turn(v) for v in sums])
    put_rows(main, m, sums)


def get_box(pair, at):
    main, side = pair
    rows = pl.ds(at, 8)
    seq = [side[m, rows, :] for m in range(4, 8)]
    seq += [main[m, rows, :] for m in range(8)]
    seq += [side[m, rows, :] for m in range(4)]
    return col_window(seq)


def over_steps(body, each=UNROLL):
    def step(i, carry):
        for e in range(each):
            k = each * i + e
            body(k, pl.multiple_of(8 * k, 8))
        return carry

    lax.fori_loop(0, STEPS // each, step, 0)
    for k in range(STEPS // each * each, STEPS):
        body(k, 8 * k)


def split3(value):
    hi = value.astype(BF16).astype(F32)
    rest = value - hi
    mid = rest.astype(BF16).astype(F32)
    return hi, mid, rest - mid


def exchange_stage(source, target, lead, bit, blocks, first, each):
    lane = lax.broadcasted_iota(jnp.int32, (8, 128), 1)
    span = 16 << bit
    upper = (lane & span) != 0

    def step(s, carry):
        for e in range(each):
            at = pl.ds(pl.multiple_of(8 * (s * each + e), 8) + first, 8)
            for which in lead:
                for m in range(TILES):
                    if m & (1 << bit):
                        continue
                    lo, hi = which + (m, at), which + (m | (1 << bit), at)
                    a, b = source[lo], source[hi]
                    target[lo] = jnp.where(upper, pltpu.roll(b, span, 1), a)
                    target[hi] = jnp.where(upper, b, pltpu.roll(a, 128 - span, 1))
        return carry

    lax.fori_loop(0, blocks // each, step, 0)


def to_blocked(work, other, blocks):
    exchange_stage(work, other, [()], 0, blocks, 0, blocks)
    exchange_stage(other, work, [()], 1, blocks, 0, blocks)
    exchange_stage(work, other, [()], 2, blocks, 0, blocks)


def grouped_lanes():
    lane = lax.broadcasted_iota(jnp.int32, (8, 128), 1)
    return 8 * (lane % 16) + lane // 16


def table_rows(line, shift, tap):
    row = lax.broadcasted_iota(jnp.int32, (8, 128), 0)
    hi, mid, lo = split3(pltpu.roll(line, HALO, 1))
    zero = jnp.zeros((8, 128), F32)
    full = jnp.where(row == 0, hi, jnp.where(row == 1, mid, jnp.where(row == 2, lo, zero)))
    if tap == 0:
        full = jnp.where(row == 3, shift, full)
    return full


def halo_kernel(shift_ref, img_hbm, weights_hbm, first_ref, second_ref, edge, weights, work, other, sems):
    moves = [
        pltpu.make_async_copy(img_hbm.at[0, pl.ds(0, EDGE)], edge.at[0], sems.at[0]),
        pltpu.make_async_copy(img_hbm.at[0, pl.ds(128 - EDGE, EDGE)], edge.at[1], sems.at[1]),
        pltpu.make_async_copy(weights_hbm.at[0], weights, sems.at[2]),
    ]
    for move in moves:
        move.start()
    for move in moves:
        move.wait()
    pick = grouped_lanes()
    for j in range(TILES):
        for side in range(2):
            tile = edge[side, :, 128 * j : 128 * j + 128].astype(F32)
            for b in range(3):
                work[j, 24 * side + 8 * b : 24 * side + 8 * b + 8, :] = jnp.take_along_axis(
                    tile[8 * b : 8 * b + 8], pick, axis=1
                )
    to_blocked(work, other, 6)
    lane = lax.broadcasted_iota(jnp.int32, (8, 128), 1)
    zero = jnp.zeros((8, 128), F32)
    shift = jnp.broadcast_to(shift_ref[0:1, :], (8, 128))
    even = lax.axis_index("strip") % 2 == 0

    def fill(up_ref, down_ref):
        for m in range(TILES):
            cols = slice(128 * m, 128 * m + 128)
            down_ref[0:EDGE, cols] = other[m, 0:EDGE, :].astype(BF16)
            up_ref[0:EDGE, cols] = other[m, EDGE : 2 * EDGE, :].astype(BF16)
        for tap in range(TAPS):
            line = jnp.broadcast_to(weights[tap : tap + 1, :], (8, 128))
            full = table_rows(line, shift, tap)
            at = 256 * tap
            up_ref[EDGE:BLOCK, at : at + 128] = jnp.where(lane < HALO, full, zero).astype(BF16)
            up_ref[EDGE:BLOCK, at + 128 : at + 256] = zero.astype(BF16)
            down_ref[EDGE:BLOCK, at : at + 128] = zero.astype(BF16)
            down_ref[EDGE:BLOCK, at + 128 : at + 256] = jnp.where(
                (lane >= HALO) & (lane < 2 * HALO), full, zero
            ).astype(BF16)

    @pl.when(even)
    def _():
        fill(first_ref, second_ref)

    @pl.when(jnp.logical_not(even))
    def _():
        fill(second_ref, first_ref)


def prep_kernel(img_ref, small_ref, own_ref, img_out, taps_out, work, other):
    shift = jnp.broadcast_to(small_ref[8:9, 0:128], (8, 128))
    lane = lax.broadcasted_iota(jnp.int32, (8, 128), 1)
    zero = jnp.zeros((8, 128), F32)
    pick = grouped_lanes()
    for j in range(TILES):
        cols = slice(128 * j, 128 * j + 128)
        tile = img_ref[:, cols].astype(F32)
        for b in range(16):
            work[j, 8 * b : 8 * b + 8, :] = jnp.take_along_axis(tile[8 * b : 8 * b + 8], pick, axis=1)
        work[j, 128:136, :] = jnp.take_along_axis(small_ref[0:8, cols], pick, axis=1)
    to_blocked(work, other, 17)
    for m in range(TILES):
        img_out[:, 128 * m : 128 * m + 128] = other[m, 0:128, :].astype(BF16)
        taps_out[m] = other[m, 128:136, :]
    for tap in range(TAPS):
        line = jnp.broadcast_to(small_ref[4 + tap : 5 + tap, 0:128], (8, 128))
        full = table_rows(line, shift, tap)
        at = 256 * tap
        own_ref[:, at : at + 128] = jnp.where(lane >= HALO, full, zero).astype(BF16)
        own_ref[:, at + 128 : at + 256] = jnp.where(lane < HALO, full, zero).astype(BF16)


def warp_kernel(shift_ref, img_ref, first_ref, second_ref, own_ref, taps_ref, out_ref, row_warped, virtual):
    even = lax.axis_index("strip") % 2 == 0
    first, second = first_ref[...], second_ref[...]
    low = jnp.where(even, second, first)
    high = jnp.where(even, first, second)
    meta = (first[EDGE:].astype(F32) + own_ref[...].astype(F32) + second[EDGE:].astype(F32)).astype(BF16)
    place = lax.broadcasted_iota(jnp.int32, (EXT, 256), 0)
    rho = (place % 8) * STEPS + place // 8
    spread = jnp.where(
        rho == lax.broadcasted_iota(jnp.int32, (EXT, 256), 1), jnp.float32(1), jnp.float32(0)
    ).astype(BF16)
    columns = [
        lax.dot_general(
            spread,
            meta[:, 256 * tap : 256 * tap + 256],
            (((1,), (1,)), ((), ())),
            preferred_element_type=F32,
        )
        for tap in range(TAPS)
    ]
    width = 2 * BLOCK + 128
    lane = lax.broadcasted_iota(jnp.int32, (EXT, width), 1)
    image_row = jnp.where(lane < EDGE, lane - EDGE, jnp.where(lane < BLOCK, -1000, lane - BLOCK))
    image_row = jnp.where(lane < BLOCK + 128 + EDGE, image_row, 2000)
    own_row = lax.broadcasted_iota(jnp.int32, (EXT, width), 0)
    own_row = (own_row % 8) * STEPS + own_row // 8 - HALO
    offset = (image_row - own_row + 1).astype(F32) - columns[0][:, 3:4]
    value = jnp.zeros((EXT, width), F32)
    for tap in range(TAPS):
        weight = columns[tap][:, 0:1] + columns[tap][:, 1:2] + columns[tap][:, 2:3]
        value = jnp.where(offset == float(tap), weight, value)
    hi, mid, lo = split3(value)
    source = jnp.concatenate([low, img_ref[...], high], axis=0)
    total = jnp.zeros((EXT, 1024), F32)
    for piece in (lo, mid, hi):
        total = total + jnp.dot(piece.astype(BF16), source, preferred_element_type=F32)
    rounded = total.astype(BF16).astype(F32)
    for m in range(TILES):
        row_warped[m] = rounded[:, 128 * m : 128 * m + 128]
    first = shift_ref[0] - 1
    lane = lax.broadcasted_iota(jnp.int32, (EXT, 128), 1)
    for v in range(TILES + TAPS - 1):
        column = first + v
        tile = lax.bitwise_and(column, 7)
        far = lax.shift_right_arithmetic(column, 3)
        moved = pltpu.roll(row_warped[tile], lax.bitwise_and(-far, 127), 1)
        virtual[v] = jnp.where((lane + far >= 0) & (lane + far < 128), moved, 0.0)
    for m in range(TILES):
        terms = [taps_ref[m, t : t + 1, :] * virtual[m + t] for t in range(TAPS)]
        out_ref[m] = ((terms[0] + terms[1]) + (terms[2] + terms[3])).astype(BF16)


def inside_rows(k, plan):
    rho = (lax.broadcasted_iota(jnp.int32, (8, 128), 0) * STEPS + k).astype(F32)
    return (rho >= plan[6:7, :]) & (rho < plan[7:8, :])


def own_stats(x_ref, plan, x_wide, sum_x, root_x, slope_r, slope_c, boxes):
    def rows(m, turn):
        value = x_ref[m].astype(F32)
        x_wide[m] = value
        steps = steps_of(value)
        put_box(boxes[0], m, turn, steps)
        put_box(boxes[1], m, turn, steps_of(value * value))
        put_rows(boxes[2][1], m, [turn(v) for v in steps])
        seq = [pltpu.roll(steps[-1], 1, 0)] + steps + [pltpu.roll(steps[0], SUBS - 1, 0)]
        put_rows(slope_r, m, [(seq[k + 2] - seq[k]) for k in range(STEPS)])

    over_tiles(rows)

    def cols(k, at):
        s1 = get_box(boxes[0], at)
        s2 = get_box(boxes[1], at)
        scale = jnp.where(inside_rows(k, plan), -0.5 / 9.0, 0.0)
        rows = pl.ds(at, 8)
        x = [boxes[2][1][7, rows, :]] + [x_wide[m, rows, :] for m in range(8)] + [boxes[2][1][0, rows, :]]
        for m in range(TILES):
            sum_x[m, rows, :] = s1[m]
            root_x[m, rows, :] = lax.rsqrt(s2[m] - s1[m] * s1[m] * (1.0 / CELLS) + 0.25 * CELLS)
            slope_r[m, rows, :] = slope_r[m, rows, :] * scale
            slope_c[m, rows, :] = (x[m + 2] - x[m]) * scale

    over_steps(cols)


def add_pair(y_ref, which, plan, first, x_wide, sum_x, root_x, sum_g, sum_h, sum_t, y_wide, coef, boxes):
    def rows(m, turn):
        value = y_ref[m].astype(F32)
        y_wide[m] = value
        put_box(boxes[0], m, turn, steps_of(value))
        put_box(boxes[1], m, turn, steps_of(value * value))
        put_box(boxes[2], m, turn, steps_of(value * x_wide[m]))

    over_tiles(rows)

    def cols(k, at):
        scale = jnp.where(inside_rows(k, plan), plan[which : which + 1, :], 0.0)
        s1 = get_box(boxes[0], at)
        s2 = get_box(boxes[1], at)
        s3 = get_box(boxes[2], at)
        for m in range(TILES):
            here = (m, pl.ds(at, 8), slice(None))
            mean = s1[m] * (1.0 / CELLS)
            root = lax.rsqrt(s2[m] - s1[m] * mean + 0.25 * CELLS)
            cov = s3[m] - sum_x[here] * mean
            u = scale * root_x[here] * root
            coef[here] = u
            g, h = u * cov, u * s1[m]
            sum_g[here] = g if first else sum_g[here] + g
            sum_h[here] = h if first else sum_h[here] + h

    over_steps(cols)

    def rows_2(m, turn):
        put_box(boxes[0], m, turn, steps_of(coef[m]))

    over_tiles(rows_2)

    def cols_2(k, at):
        s1 = get_box(boxes[0], at)
        for m in range(TILES):
            here = (m, pl.ds(at, 8), slice(None))
            t = y_wide[here] * s1[m]
            sum_t[here] = t if first else sum_t[here] + t

    over_steps(cols_2)


def restore(natural, other, which, target):
    lead = [(w,) for w in which]
    exchange_stage(natural, other, lead, 0, 16, HALO, EACH // len(which))
    exchange_stage(other, natural, lead, 1, 16, HALO, EACH // len(which))
    exchange_stage(natural, other, lead, 2, 16, HALO, EACH // len(which))
    lane = lax.broadcasted_iota(jnp.int32, (8, 128), 1)
    pick = (lane % 8) * 16 + lane // 8
    each = EACH // len(which)

    def step(s, carry):
        for e in range(each):
            at = pl.multiple_of(8 * (each * s + e), 8)
            for w in which:
                for j in range(TILES):
                    tile = jnp.take_along_axis(other[w, j, pl.ds(at + HALO, 8), :], pick, axis=1)
                    target[w, pl.ds(at, 8), 128 * j : 128 * j + 128] = tile
        return carry

    lax.fori_loop(0, 16 // each, step, 0)


def finish(x_wide, sum_x, root_x, slope_r, slope_c, sum_g, sum_h, sum_t, natural, other, wide, sems, grad_hbm, disp_hbm, boxes):
    def rows(m, turn):
        root = root_x[m]
        g = root * root * sum_g[m]
        put_box(boxes[0], m, turn, steps_of(sum_h[m] - g * sum_x[m]))
        put_box(boxes[1], m, turn, steps_of(g))

    over_tiles(rows)

    def cols(k, at):
        s1 = get_box(boxes[0], at)
        s2 = get_box(boxes[1], at)
        for m in range(TILES):
            here = (m, pl.ds(at, 8), slice(None))
            grad = s1[m] * (1.0 / CELLS) + x_wide[here] * s2[m] - sum_t[here]
            natural[0, m, pl.ds(k, 8, stride=STEPS), :] = grad
            sum_g[here] = grad * slope_r[here]
            sum_h[here] = grad * slope_c[here]

    over_steps(cols)
    restore(natural, other, [0], wide)
    out = pltpu.make_async_copy(wide.at[0], grad_hbm, sems.at[0])
    out.start()

    def rows_2(m, turn):
        put_box(boxes[0], m, turn, steps_of(sum_g[m]))
        put_box(boxes[1], m, turn, steps_of(sum_h[m]))

    over_tiles(rows_2)

    def cols_2(k, at):
        s1 = get_box(boxes[0], at)
        s2 = get_box(boxes[1], at)
        for m in range(TILES):
            natural[1, m, pl.ds(k, 8, stride=STEPS), :] = s1[m]
            natural[2, m, pl.ds(k, 8, stride=STEPS), :] = s2[m]

    over_steps(cols_2)
    restore(natural, other, [1, 2], wide)
    out_2 = pltpu.make_async_copy(wide.at[pl.ds(1, 2)], disp_hbm, sems.at[1])
    out_2.start()
    out.wait()
    out_2.wait()


def others(own):
    way = 1 - 2 * (own % 2)
    return [own + way, own + 2 * way, own - way, own - 2 * way, own - 3 * way, own + 3 * way]


def field():
    return pltpu.VMEM((TILES, EXT, 128), F32)


def shape(dims, kind):
    return jax.ShapeDtypeStruct(dims, kind)


FIELD = shape((TILES, EXT, 128), F32)


def own_kernel(small, x, x_wide, sum_x, root_x, slope_r, slope_c, plan, *boxes):
    own, strip = lax.axis_index("sec"), lax.axis_index("strip")
    row = lax.broadcasted_iota(jnp.int32, (8, 128), 0)
    lane = lax.broadcasted_iota(jnp.int32, (8, 128), 1)
    table = small[8:16, 0:128]
    lines = jnp.where(row == 6, jnp.where(strip == 0, HALO, 0), jnp.where(strip == 15, HALO + 128, EXT)).astype(F32)
    for i, section in enumerate(others(own)):
        low, gap = jnp.minimum(own, section), jnp.abs(own - section)
        here = (row == gap) & (lane == low) & (section >= 0) & (section < 16)
        weight = jnp.sum(jnp.sum(jnp.where(here, table, 0.0), axis=1, keepdims=True), axis=0, keepdims=True)
        lines = jnp.where(row == i, weight, lines)
    plan[...] = lines
    own_stats(x, lines, x_wide, sum_x, root_x, slope_r, slope_c, paired(boxes))


def paired(refs):
    return [(refs[2 * i], refs[2 * i + 1]) for i in range(3)]


def pair_kernel(turns, plan, *refs):
    ys, refs = refs[: len(turns)], refs[len(turns) :]
    first = 0 in turns
    kept = 0 if first else 3
    x_wide, sum_x, root_x = refs[:3]
    g, h, t = refs[3 + kept : 6 + kept]
    y_wide, coef = refs[6 + kept : 8 + kept]
    boxes = paired(refs[8 + kept :])
    for i, y in zip(turns, ys):
        add_pair(y, i, plan[...], i == 0, x_wide, sum_x, root_x, g, h, t, y_wide, coef, boxes)


def last_kernel(turns, plan, *refs):
    ys, refs = refs[: len(turns)], refs[len(turns) :]
    x_wide, sum_x, root_x, slope_r, slope_c, _, _, _, grad, disp, g, h, t, y_wide, coef, natural, other, wide, sems = refs[:19]
    boxes = paired(refs[19:])
    for i, y in zip(turns, ys):
        add_pair(y, i, plan[...], False, x_wide, sum_x, root_x, g, h, t, y_wide, coef, boxes)
    finish(x_wide, sum_x, root_x, slope_r, slope_c, g, h, t, natural, other, wide, sems, grad, disp, boxes)


def last_scratch():
    three = pltpu.VMEM((3, TILES, EXT, 128), F32)
    wide = pltpu.VMEM((3, 128, 1024), F32)
    return [field(), field(), three, three, wide, pltpu.SemaphoreType.DMA((2,))] + [field() for _ in range(6)]


def params(mib=24):
    return pltpu.CompilerParams(vmem_limit_bytes=mib * 1024 * 1024)


def cost(us):
    return pl.CostEstimate(flops=int(us * 4_000_000), bytes_accessed=1_000_000, transcendentals=0)


def add_pairs(turns, plan, ys, stats, sums):
    ins = [plan, *ys, *stats, *sums]
    start = len(ins) - len(sums)
    return pl.pallas_call(
        functools.partial(pair_kernel, turns),
        out_shape=(FIELD,) * 3,
        in_specs=[VMEM] * len(ins),
        out_specs=(VMEM,) * 3,
        scratch_shapes=[field() for _ in range(8)],
        input_output_aliases={start + i: i for i in range(len(sums))},
        compiler_params=params(),
        cost_estimate=cost(1.5 * len(turns)),
        name="pair",
    )(*ins)


def per_device(images, row_weights, row_shift, col_weights, col_shift, pair_on):
    block = shape((BLOCK, 1024), BF16)

    def wide(value):
        return jnp.pad(value.astype(F32), ((0, 0), (0, 1024 - value.shape[1])))

    small = jnp.concatenate(
        [
            col_weights[0].astype(F32),
            wide(row_weights[0]),
            jnp.broadcast_to(row_shift.astype(F32), (1, 1024)),
            wide(pair_on.T),
            jnp.zeros((4, 1024), F32),
        ]
    )
    halo = pl.pallas_call(
        halo_kernel,
        out_shape=(block, block),
        in_specs=[VMEM, HBM, HBM],
        out_specs=(VMEM,) * 2,
        scratch_shapes=[
            pltpu.VMEM((2, EDGE, 1024), BF16),
            pltpu.VMEM((TAPS, 128), F32),
            pltpu.VMEM((TILES, 48, 128), F32),
            pltpu.VMEM((TILES, 48, 128), F32),
            pltpu.SemaphoreType.DMA((3,)),
        ],
        compiler_params=pltpu.CompilerParams(vmem_limit_bytes=66_500_000),
        name="halo",
    )(jnp.broadcast_to(row_shift.astype(F32), (8, 128)), images, row_weights)
    strips = range(16)

    def swap(value, step):
        pairs = [(s, s + step * (1 - 2 * (s % 2))) for s in strips]
        return lax.ppermute(value, "strip", [p for p in pairs if 0 <= p[1] < 16])

    first = swap(halo[0], 1)
    second = swap(halo[1], -1)
    own, image, taps = pl.pallas_call(
        prep_kernel,
        out_shape=(shape((8, 1024), BF16), shape((128, 1024), BF16), shape((TILES, 8, 128), F32)),
        in_specs=[VMEM] * 2,
        out_specs=(VMEM,) * 3,
        scratch_shapes=[pltpu.VMEM((TILES, 136, 128), F32)] * 2,
        compiler_params=params(),
        cost_estimate=cost(1),
        name="prep",
    )(images[0], small)
    warped = pl.pallas_call(
        warp_kernel,
        out_shape=shape((TILES, EXT, 128), BF16),
        in_specs=[SMEM] + [VMEM] * 5,
        out_specs=VMEM,
        scratch_shapes=[field(), pltpu.VMEM((TILES + TAPS - 1, EXT, 128), F32)],
        compiler_params=params(),
        name="warp",
    )(col_shift, image, first, second, own, taps)
    sections = range(16)

    def send(value, target):
        pairs = [(s, target(s, 1 - 2 * (s % 2))) for s in sections]
        return lax.ppermute(value, "sec", [p for p in pairs if 0 <= p[1] < 16])

    from_0 = send(warped, lambda s, way: s + way)
    from_1 = send(warped, lambda s, way: s - 2 * way)
    from_2 = send(from_1, lambda s, way: s + way)
    from_3 = send(warped, lambda s, way: s + 2 * way)
    from_4 = send(from_1, lambda s, way: s - way)
    from_5 = send(from_3, lambda s, way: s + way)
    x_wide, sum_x, root_x, slope_r, slope_c, plan = pl.pallas_call(
        own_kernel,
        out_shape=(FIELD,) * 5 + (shape((8, 128), F32),),
        in_specs=[VMEM, VMEM],
        out_specs=(VMEM,) * 6,
        scratch_shapes=[field() for _ in range(6)],
        compiler_params=params(),
        cost_estimate=cost(1.3),
        name="own",
    )(small, warped)
    stats = (x_wide, sum_x, root_x)
    sums = ()
    for i, y in enumerate((from_0, from_1, from_2, from_3, from_4)):
        sums = add_pairs((i,), plan, (y,), stats, sums)
    grad, disp = pl.pallas_call(
        functools.partial(last_kernel, (5,)),
        out_shape=(shape((128, 1024), F32), shape((2, 128, 1024), F32)) + (FIELD,) * 3,
        in_specs=[VMEM] * 10,
        out_specs=(HBM, HBM) + (VMEM,) * 3,
        scratch_shapes=last_scratch(),
        input_output_aliases={7: 2, 8: 3, 9: 4},
        compiler_params=params(),
        cost_estimate=cost(5),
        name="last",
    )(plan, from_5, *stats, slope_r, slope_c, *sums)[:2]
    return grad[None], disp[:, None]


def solution(mesh):
    return jax.shard_map(
        per_device,
        mesh=mesh,
        in_specs=(
            P("sec", "strip", None),
            P("sec", None, "strip"),
            P("sec", "strip"),
            P("sec", None, None),
            P("sec"),
            P(),
        ),
        out_specs=(P("sec", "strip", None), P(None, "sec", "strip", None)),
        check_vma=False,
    )
```

```python
import functools

import jax
import jax.numpy as jnp
from jax import lax
from jax.experimental import pallas as pl
from jax.experimental.pallas import tpu as pltpu
from jax.sharding import PartitionSpec as P


TAPS = 4
HALO = 12
STEPS = 19
SUBS = 8
EXT = STEPS * SUBS
TILES = 8
CELLS = 81.0
F32 = jnp.float32
BF16 = jnp.bfloat16
VMEM = pl.BlockSpec(memory_space=pltpu.VMEM)
SMEM = pl.BlockSpec(memory_space=pltpu.SMEM)
HBM = pl.BlockSpec(memory_space=pl.ANY)
EDGE = 24
UNROLL = 3
GROUP = 8
BLOCK = 32


def window_sums(seq, width):
    count = len(seq) - width + 1
    out = [None] * count
    for base in range(0, count, width):
        suffix = [None] * width
        suffix[width - 1] = seq[base + width - 1]
        for i in range(width - 2, -1, -1):
            suffix[i] = seq[base + i] + suffix[i + 1]
        prefix = None
        for i in range(width):
            if base + i >= count:
                break
            if i == 0:
                out[base] = suffix[0]
            else:
                nxt = seq[base + width + i - 1]
                prefix = nxt if prefix is None else prefix + nxt
                out[base + i] = suffix[i] + prefix
    return out


def row_window(steps):
    low = [pltpu.roll(v, 1, 0) for v in steps[-4:]]
    high = [pltpu.roll(v, SUBS - 1, 0) for v in steps[:4]]
    return window_sums(low + steps + high, 9)


def col_window(seq):
    suffix = [None] * 8
    suffix[7] = seq[7]
    for i in range(6, -1, -1):
        suffix[i] = seq[i] + suffix[i + 1]
    out = []
    prefix = None
    for i in range(8):
        prefix = seq[8 + i] if prefix is None else prefix + seq[8 + i]
        out.append(suffix[i] + prefix)
    return out


def steps_of(value):
    return [value[8 * k : 8 * k + 8] for k in range(STEPS)]


def put_rows(ref, tile, values):
    for k, v in enumerate(values):
        ref[tile, 8 * k : 8 * k + 8, :] = v


def over_tiles(body, each=GROUP):
    lane = lax.broadcasted_iota(jnp.int32, (8, 128), 1)

    def turn_to(shift, edge):
        keep = lane != edge
        return lambda v: jnp.where(keep, pltpu.roll(v, shift, 1), 0.0)

    if each == TILES:
        for m in range(TILES):
            body(m, turn_to(127, 127) if m < 4 else turn_to(1, 0))
        return

    def part(q, carry):
        low = each * q < 4
        turn = turn_to(jnp.where(low, 127, 1), jnp.where(low, 127, 0))
        for i in range(each):
            body(each * q + i, turn)
        return carry

    lax.fori_loop(0, TILES // each, part, 0)


def put_box(pair, m, turn, values):
    main, side = pair
    sums = row_window(values)
    put_rows(side, m, [turn(v) for v in sums])
    put_rows(main, m, sums)


def get_box(pair, at):
    main, side = pair
    rows = pl.ds(at, 8)
    seq = [side[m, rows, :] for m in range(4, 8)]
    seq += [main[m, rows, :] for m in range(8)]
    seq += [side[m, rows, :] for m in range(4)]
    return col_window(seq)


def over_steps(body, each=UNROLL):
    def step(i, carry):
        for e in range(each):
            k = each * i + e
            body(k, pl.multiple_of(8 * k, 8))
        return carry

    lax.fori_loop(0, STEPS // each, step, 0)
    for k in range(STEPS // each * each, STEPS):
        body(k, 8 * k)


def split3(value):
    hi = value.astype(BF16).astype(F32)
    rest = value - hi
    mid = rest.astype(BF16).astype(F32)
    return hi, mid, rest - mid


def exchange_stage(source, target, lead, bit, blocks, first, each):
    lane = lax.broadcasted_iota(jnp.int32, (8, 128), 1)
    span = 16 << bit
    upper = (lane & span) != 0

    def step(s, carry):
        for e in range(each):
            at = pl.ds(pl.multiple_of(8 * (s * each + e), 8) + first, 8)
            for which in lead:
                for m in range(TILES):
                    if m & (1 << bit):
                        continue
                    lo, hi = which + (m, at), which + (m | (1 << bit), at)
                    a, b = source[lo], source[hi]
                    target[lo] = jnp.where(upper, pltpu.roll(b, span, 1), a)
                    target[hi] = jnp.where(upper, b, pltpu.roll(a, 128 - span, 1))
        return carry

    lax.fori_loop(0, blocks // each, step, 0)


def to_blocked(work, other, blocks):
    exchange_stage(work, other, [()], 0, blocks, 0, blocks)
    exchange_stage(other, work, [()], 1, blocks, 0, blocks)
    exchange_stage(work, other, [()], 2, blocks, 0, blocks)


def grouped_lanes():
    lane = lax.broadcasted_iota(jnp.int32, (8, 128), 1)
    return 8 * (lane % 16) + lane // 16


def table_rows(line, shift, tap):
    row = lax.broadcasted_iota(jnp.int32, (8, 128), 0)
    hi, mid, lo = split3(pltpu.roll(line, HALO, 1))
    zero = jnp.zeros((8, 128), F32)
    full = jnp.where(row == 0, hi, jnp.where(row == 1, mid, jnp.where(row == 2, lo, zero)))
    if tap == 0:
        full = jnp.where(row == 3, shift, full)
    return full


def halo_kernel(shift_ref, img_hbm, weights_hbm, first_ref, second_ref, edge, weights, work, other, sems):
    moves = [
        pltpu.make_async_copy(img_hbm.at[0, pl.ds(0, EDGE)], edge.at[0], sems.at[0]),
        pltpu.make_async_copy(img_hbm.at[0, pl.ds(128 - EDGE, EDGE)], edge.at[1], sems.at[1]),
        pltpu.make_async_copy(weights_hbm.at[0], weights, sems.at[2]),
    ]
    for move in moves:
        move.start()
    for move in moves:
        move.wait()
    pick = grouped_lanes()
    for j in range(TILES):
        for side in range(2):
            tile = edge[side, :, 128 * j : 128 * j + 128].astype(F32)
            for b in range(3):
                work[j, 24 * side + 8 * b : 24 * side + 8 * b + 8, :] = jnp.take_along_axis(
                    tile[8 * b : 8 * b + 8], pick, axis=1
                )
    to_blocked(work, other, 6)
    lane = lax.broadcasted_iota(jnp.int32, (8, 128), 1)
    zero = jnp.zeros((8, 128), F32)
    shift = jnp.full((8, 128), shift_ref[0, 0], jnp.int32).astype(F32)
    even = lax.axis_index("strip") % 2 == 0

    def fill(up_ref, down_ref):
        for m in range(TILES):
            cols = slice(128 * m, 128 * m + 128)
            down_ref[0:EDGE, cols] = other[m, 0:EDGE, :].astype(BF16)
            up_ref[0:EDGE, cols] = other[m, EDGE : 2 * EDGE, :].astype(BF16)
        for tap in range(TAPS):
            line = jnp.broadcast_to(weights[tap : tap + 1, :], (8, 128))
            full = table_rows(line, shift, tap)
            at = 256 * tap
            up_ref[EDGE:BLOCK, at : at + 128] = jnp.where(lane < HALO, full, zero).astype(BF16)
            up_ref[EDGE:BLOCK, at + 128 : at + 256] = zero.astype(BF16)
            down_ref[EDGE:BLOCK, at : at + 128] = zero.astype(BF16)
            down_ref[EDGE:BLOCK, at + 128 : at + 256] = jnp.where(
                (lane >= HALO) & (lane < 2 * HALO), full, zero
            ).astype(BF16)

    @pl.when(even)
    def _():
        fill(first_ref, second_ref)

    @pl.when(jnp.logical_not(even))
    def _():
        fill(second_ref, first_ref)


def prep_kernel(img_ref, small_ref, own_ref, img_out, taps_out, order, work, other):
    order[...] = column_order()
    shift = jnp.broadcast_to(small_ref[8:9, 0:128], (8, 128))
    lane = lax.broadcasted_iota(jnp.int32, (8, 128), 1)
    zero = jnp.zeros((8, 128), F32)
    pick = grouped_lanes()
    for j in range(TILES):
        cols = slice(128 * j, 128 * j + 128)
        tile = img_ref[:, cols].astype(F32)
        for b in range(16):
            work[j, 8 * b : 8 * b + 8, :] = jnp.take_along_axis(tile[8 * b : 8 * b + 8], pick, axis=1)
        work[j, 128:136, :] = jnp.take_along_axis(small_ref[0:8, cols], pick, axis=1)
    to_blocked(work, other, 17)
    for m in range(TILES):
        img_out[:, 128 * m : 128 * m + 128] = other[m, 0:128, :].astype(BF16)
        taps_out[m] = other[m, 128:136, :]
    for tap in range(TAPS):
        line = jnp.broadcast_to(small_ref[4 + tap : 5 + tap, 0:128], (8, 128))
        full = table_rows(line, shift, tap)
        at = 256 * tap
        own_ref[:, at : at + 128] = jnp.where(lane >= HALO, full, zero).astype(BF16)
        own_ref[:, at + 128 : at + 256] = jnp.where(lane < HALO, full, zero).astype(BF16)


def warp_kernel(shift_ref, img_ref, first_ref, second_ref, own_ref, taps_ref, out_ref, row_warped, virtual):
    even = lax.axis_index("strip") % 2 == 0
    first, second = first_ref[...], second_ref[...]
    low = jnp.where(even, second, first)
    high = jnp.where(even, first, second)
    meta = (first[EDGE:].astype(F32) + own_ref[...].astype(F32) + second[EDGE:].astype(F32)).astype(BF16)
    place = lax.broadcasted_iota(jnp.int32, (EXT, 256), 0)
    rho = (place % 8) * STEPS + place // 8
    spread = jnp.where(
        rho == lax.broadcasted_iota(jnp.int32, (EXT, 256), 1), jnp.float32(1), jnp.float32(0)
    ).astype(BF16)
    columns = [
        lax.dot_general(
            spread,
            meta[:, 256 * tap : 256 * tap + 256],
            (((1,), (1,)), ((), ())),
            preferred_element_type=F32,
        )
        for tap in range(TAPS)
    ]
    width = 2 * BLOCK + 128
    lane = lax.broadcasted_iota(jnp.int32, (EXT, width), 1)
    image_row = jnp.where(lane < EDGE, lane - EDGE, jnp.where(lane < BLOCK, -1000, lane - BLOCK))
    image_row = jnp.where(lane < BLOCK + 128 + EDGE, image_row, 2000)
    own_row = lax.broadcasted_iota(jnp.int32, (EXT, width), 0)
    own_row = (own_row % 8) * STEPS + own_row // 8 - HALO
    offset = (image_row - own_row + 1).astype(F32) - columns[0][:, 3:4]
    value = jnp.zeros((EXT, width), F32)
    for tap in range(TAPS):
        weight = columns[tap][:, 0:1] + columns[tap][:, 1:2] + columns[tap][:, 2:3]
        value = jnp.where(offset == float(tap), weight, value)
    hi, mid, lo = split3(value)
    source = jnp.concatenate([low, img_ref[...], high], axis=0)
    total = jnp.zeros((EXT, 1024), F32)
    for piece in (lo, mid, hi):
        total = total + jnp.dot(piece.astype(BF16), source, preferred_element_type=F32)
    rounded = total.astype(BF16).astype(F32)
    for m in range(TILES):
        row_warped[m] = rounded[:, 128 * m : 128 * m + 128]
    first = shift_ref[0] - 1
    lane = lax.broadcasted_iota(jnp.int32, (EXT, 128), 1)
    for v in range(TILES + TAPS - 1):
        column = first + v
        tile = lax.bitwise_and(column, 7)
        far = lax.shift_right_arithmetic(column, 3)
        moved = pltpu.roll(row_warped[tile], lax.bitwise_and(-far, 127), 1)
        virtual[v] = jnp.where((lane + far >= 0) & (lane + far < 128), moved, 0.0)
    for m in range(TILES):
        terms = [taps_ref[m, t : t + 1, :] * virtual[m + t] for t in range(TAPS)]
        out_ref[m] = ((terms[0] + terms[1]) + (terms[2] + terms[3])).astype(BF16)


def inside_rows(k, plan):
    rho = (lax.broadcasted_iota(jnp.int32, (8, 128), 0) * STEPS + k).astype(F32)
    return (rho >= plan[6:7, :]) & (rho < plan[7:8, :])


def own_stats(x_ref, plan, x_wide, sum_x, root_x, slope_r, slope_c, boxes):
    def rows(m, turn):
        value = x_ref[m].astype(F32)
        x_wide[m] = value
        steps = steps_of(value)
        put_box(boxes[0], m, turn, steps)
        put_box(boxes[1], m, turn, steps_of(value * value))
        put_rows(boxes[2][1], m, [turn(v) for v in steps])
        seq = [pltpu.roll(steps[-1], 1, 0)] + steps + [pltpu.roll(steps[0], SUBS - 1, 0)]
        put_rows(slope_r, m, [(seq[k + 2] - seq[k]) for k in range(STEPS)])

    over_tiles(rows)

    def cols(k, at):
        s1 = get_box(boxes[0], at)
        s2 = get_box(boxes[1], at)
        scale = jnp.where(inside_rows(k, plan), -0.5 / 9.0, 0.0)
        rows = pl.ds(at, 8)
        x = [boxes[2][1][7, rows, :]] + [x_wide[m, rows, :] for m in range(8)] + [boxes[2][1][0, rows, :]]
        for m in range(TILES):
            sum_x[m, rows, :] = s1[m]
            root_x[m, rows, :] = lax.rsqrt(s2[m] - s1[m] * s1[m] * (1.0 / CELLS) + 0.25 * CELLS)
            slope_r[m, rows, :] = slope_r[m, rows, :] * scale
            slope_c[m, rows, :] = (x[m + 2] - x[m]) * scale

    over_steps(cols)


def add_pair(y_ref, which, plan, first, x_wide, sum_x, root_x, sum_g, sum_h, sum_t, y_wide, coef, boxes):
    def rows(m, turn):
        value = y_ref[m].astype(F32)
        y_wide[m] = value
        steps = steps_of(value)
        turned = [turn(v) for v in steps]
        put_rows(boxes[0][0], m, row_window(steps))
        put_rows(boxes[1][0], m, row_window([v * v for v in steps]))
        put_rows(boxes[0][1], m, row_window(turned))
        put_rows(boxes[1][1], m, row_window([v * v for v in turned]))
        put_box(boxes[2], m, turn, steps_of(value * x_wide[m]))

    over_tiles(rows)

    def cols(k, at):
        scale = jnp.where(inside_rows(k, plan), plan[which : which + 1, :], 0.0)
        s1 = get_box(boxes[0], at)
        s2 = get_box(boxes[1], at)
        s3 = get_box(boxes[2], at)
        for m in range(TILES):
            here = (m, pl.ds(at, 8), slice(None))
            mean = s1[m] * (1.0 / CELLS)
            root = lax.rsqrt(s2[m] - s1[m] * mean + 0.25 * CELLS)
            cov = s3[m] - sum_x[here] * mean
            u = scale * root_x[here] * root
            coef[here] = u
            g, h = u * cov, u * s1[m]
            sum_g[here] = g if first else sum_g[here] + g
            sum_h[here] = h if first else sum_h[here] + h

    over_steps(cols)

    def rows_2(m, turn):
        put_box(boxes[0], m, turn, steps_of(coef[m]))

    over_tiles(rows_2)

    def cols_2(k, at):
        s1 = get_box(boxes[0], at)
        for m in range(TILES):
            here = (m, pl.ds(at, 8), slice(None))
            t = y_wide[here] * s1[m]
            sum_t[here] = t if first else sum_t[here] + t

    over_steps(cols_2)


def column_order():
    source = lax.broadcasted_iota(jnp.int32, (512, 512), 0)
    column = lax.broadcasted_iota(jnp.int32, (512, 512), 1)
    tile = 4 * ((source // 64) % 2) + source // 128
    return jnp.where(8 * (source % 64) + tile == column, 1.0, 0.0).astype(BF16)


def restore(natural, order, which, target):
    lane = lax.broadcasted_iota(jnp.int32, (128, 128), 1)
    upper = lane >= 64
    rows = slice(HALO, HALO + 128)
    for w in which:
        halves = [], []
        for m in range(4):
            a, b = natural[w, m, rows, :], natural[w, m + 4, rows, :]
            halves[0].append(jnp.where(upper, pltpu.roll(b, 64, 1), a))
            halves[1].append(jnp.where(upper, b, pltpu.roll(a, 64, 1)))
        for h in range(2):
            value = jnp.concatenate(halves[h], axis=1)
            hi = value.astype(BF16)
            lo = (value - hi.astype(F32)).astype(BF16)
            target[w, :, 512 * h : 512 * h + 512] = jnp.dot(
                hi, order[...], preferred_element_type=F32
            ) + jnp.dot(lo, order[...], preferred_element_type=F32)


def finish(x_wide, sum_x, root_x, slope_r, slope_c, sum_g, sum_h, sum_t, natural, order, wide, sems, grad_hbm, disp_hbm, boxes):
    def rows(m, turn):
        root = root_x[m]
        g = root * root * sum_g[m]
        put_box(boxes[0], m, turn, steps_of(sum_h[m] - g * sum_x[m]))
        put_box(boxes[1], m, turn, steps_of(g))

    over_tiles(rows)

    def cols(k, at):
        s1 = get_box(boxes[0], at)
        s2 = get_box(boxes[1], at)
        for m in range(TILES):
            here = (m, pl.ds(at, 8), slice(None))
            grad = s1[m] * (1.0 / CELLS) + x_wide[here] * s2[m] - sum_t[here]
            natural[0, m, pl.ds(k, 8, stride=STEPS), :] = grad
            sum_g[here] = grad * slope_r[here]
            sum_h[here] = grad * slope_c[here]

    over_steps(cols)
    restore(natural, order, [0], wide)
    out = pltpu.make_async_copy(wide.at[0], grad_hbm, sems.at[0])
    out.start()

    def rows_2(m, turn):
        put_box(boxes[0], m, turn, steps_of(sum_g[m]))
        put_box(boxes[1], m, turn, steps_of(sum_h[m]))

    over_tiles(rows_2)

    def cols_2(k, at):
        s1 = get_box(boxes[0], at)
        s2 = get_box(boxes[1], at)
        for m in range(TILES):
            natural[1, m, pl.ds(k, 8, stride=STEPS), :] = s1[m]
            natural[2, m, pl.ds(k, 8, stride=STEPS), :] = s2[m]

    over_steps(cols_2)
    restore(natural, order, [1, 2], wide)
    out_2 = pltpu.make_async_copy(wide.at[pl.ds(1, 2)], disp_hbm, sems.at[1])
    out_2.start()
    out.wait()
    out_2.wait()


def others(own):
    way = 1 - 2 * (own % 2)
    return [own + way, own + 2 * way, own - way, own - 2 * way, own - 3 * way, own + 3 * way]


def field():
    return pltpu.VMEM((TILES, EXT, 128), F32)


def shape(dims, kind):
    return jax.ShapeDtypeStruct(dims, kind)


FIELD = shape((TILES, EXT, 128), F32)


def own_kernel(small, x, x_wide, sum_x, root_x, slope_r, slope_c, plan, *boxes):
    own, strip = lax.axis_index("sec"), lax.axis_index("strip")
    row = lax.broadcasted_iota(jnp.int32, (8, 128), 0)
    lane = lax.broadcasted_iota(jnp.int32, (8, 128), 1)
    table = small[8:16, 0:128]
    lines = jnp.where(row == 6, jnp.where(strip == 0, HALO, 0), jnp.where(strip == 15, HALO + 128, EXT)).astype(F32)
    for i, section in enumerate(others(own)):
        low, gap = jnp.minimum(own, section), jnp.abs(own - section)
        here = (row == gap) & (lane == low) & (section >= 0) & (section < 16)
        weight = jnp.sum(jnp.sum(jnp.where(here, table, 0.0), axis=1, keepdims=True), axis=0, keepdims=True)
        lines = jnp.where(row == i, weight, lines)
    plan[...] = lines
    own_stats(x, lines, x_wide, sum_x, root_x, slope_r, slope_c, paired(boxes))


def paired(refs):
    return [(refs[2 * i], refs[2 * i + 1]) for i in range(3)]


def pair_kernel(turns, plan, *refs):
    ys, refs = refs[: len(turns)], refs[len(turns) :]
    first = 0 in turns
    kept = 0 if first else 3
    x_wide, sum_x, root_x = refs[:3]
    g, h, t = refs[3 + kept : 6 + kept]
    y_wide, coef = refs[6 + kept : 8 + kept]
    boxes = paired(refs[8 + kept :])
    for i, y in zip(turns, ys):
        add_pair(y, i, plan[...], i == 0, x_wide, sum_x, root_x, g, h, t, y_wide, coef, boxes)


def last_kernel(turns, plan, *refs):
    ys, refs = refs[: len(turns)], refs[len(turns) :]
    x_wide, sum_x, root_x, slope_r, slope_c, order, _, _, _, grad, disp, g, h, t, y_wide, coef, natural, wide, sems = refs[:19]
    boxes = paired(refs[19:])
    for i, y in zip(turns, ys):
        add_pair(y, i, plan[...], False, x_wide, sum_x, root_x, g, h, t, y_wide, coef, boxes)
    finish(x_wide, sum_x, root_x, slope_r, slope_c, g, h, t, natural, order, wide, sems, grad, disp, boxes)


def last_scratch():
    three = pltpu.VMEM((3, TILES, EXT, 128), F32)
    wide = pltpu.VMEM((3, 128, 1024), F32)
    return [field(), field(), three, wide, pltpu.SemaphoreType.DMA((2,))] + [field() for _ in range(6)]


def params(mib=24):
    return pltpu.CompilerParams(vmem_limit_bytes=mib * 1024 * 1024)


def cost(us):
    return pl.CostEstimate(flops=int(us * 4_000_000), bytes_accessed=1_000_000, transcendentals=0)


def add_pairs(turns, plan, ys, stats, sums):
    ins = [plan, *ys, *stats, *sums]
    start = len(ins) - len(sums)
    return pl.pallas_call(
        functools.partial(pair_kernel, turns),
        out_shape=(FIELD,) * 3,
        in_specs=[VMEM] * len(ins),
        out_specs=(VMEM,) * 3,
        scratch_shapes=[field() for _ in range(8)],
        input_output_aliases={start + i: i for i in range(len(sums))},
        compiler_params=params(),
        cost_estimate=cost(1.5 * len(turns)),
        name="pair",
    )(*ins)


def per_device(images, row_weights, row_shift, col_weights, col_shift, pair_on):
    block = shape((BLOCK, 1024), BF16)

    def wide(value):
        return jnp.pad(value.astype(F32), ((0, 0), (0, 1024 - value.shape[1])))

    small = jnp.concatenate(
        [
            col_weights[0].astype(F32),
            wide(row_weights[0]),
            jnp.broadcast_to(row_shift.astype(F32), (1, 1024)),
            wide(pair_on.T),
            jnp.zeros((4, 1024), F32),
        ]
    )
    halo = pl.pallas_call(
        halo_kernel,
        out_shape=(block, block),
        in_specs=[SMEM, HBM, HBM],
        out_specs=(VMEM,) * 2,
        scratch_shapes=[
            pltpu.VMEM((2, EDGE, 1024), BF16),
            pltpu.VMEM((TAPS, 128), F32),
            pltpu.VMEM((TILES, 48, 128), F32),
            pltpu.VMEM((TILES, 48, 128), F32),
            pltpu.SemaphoreType.DMA((3,)),
        ],
        compiler_params=pltpu.CompilerParams(vmem_limit_bytes=66_500_000),
        name="halo",
    )(row_shift, images, row_weights)
    strips = range(16)

    def swap(value, step):
        pairs = [(s, s + step * (1 - 2 * (s % 2))) for s in strips]
        return lax.ppermute(value, "strip", [p for p in pairs if 0 <= p[1] < 16])

    first = swap(halo[0], 1)
    second = swap(halo[1], -1)
    own, image, taps, order = pl.pallas_call(
        prep_kernel,
        out_shape=(
            shape((8, 1024), BF16),
            shape((128, 1024), BF16),
            shape((TILES, 8, 128), F32),
            shape((512, 512), BF16),
        ),
        in_specs=[VMEM] * 2,
        out_specs=(VMEM,) * 4,
        scratch_shapes=[pltpu.VMEM((TILES, 136, 128), F32)] * 2,
        compiler_params=params(),
        cost_estimate=cost(1),
        name="prep",
    )(images[0], small)
    warped = pl.pallas_call(
        warp_kernel,
        out_shape=shape((TILES, EXT, 128), BF16),
        in_specs=[SMEM] + [VMEM] * 5,
        out_specs=VMEM,
        scratch_shapes=[field(), pltpu.VMEM((TILES + TAPS - 1, EXT, 128), F32)],
        compiler_params=params(),
        name="warp",
    )(col_shift, image, first, second, own, taps)
    sections = range(16)

    def send(value, target):
        pairs = [(s, target(s, 1 - 2 * (s % 2))) for s in sections]
        return lax.ppermute(value, "sec", [p for p in pairs if 0 <= p[1] < 16])

    from_0 = send(warped, lambda s, way: s + way)
    from_1 = send(warped, lambda s, way: s - 2 * way)
    from_2 = send(from_1, lambda s, way: s + way)
    from_3 = send(warped, lambda s, way: s + 2 * way)
    from_4 = send(from_1, lambda s, way: s - way)
    from_5 = send(from_3, lambda s, way: s + way)
    x_wide, sum_x, root_x, slope_r, slope_c, plan = pl.pallas_call(
        own_kernel,
        out_shape=(FIELD,) * 5 + (shape((8, 128), F32),),
        in_specs=[VMEM, VMEM],
        out_specs=(VMEM,) * 6,
        scratch_shapes=[field() for _ in range(6)],
        compiler_params=params(),
        cost_estimate=cost(1.3),
        name="own",
    )(small, warped)
    stats = (x_wide, sum_x, root_x)
    sums = ()
    for i, y in enumerate((from_0, from_1, from_2, from_3, from_4)):
        sums = add_pairs((i,), plan, (y,), stats, sums)
    grad, disp = pl.pallas_call(
        functools.partial(last_kernel, (5,)),
        out_shape=(shape((128, 1024), F32), shape((2, 128, 1024), F32)) + (FIELD,) * 3,
        in_specs=[VMEM] * 11,
        out_specs=(HBM, HBM) + (VMEM,) * 3,
        scratch_shapes=last_scratch(),
        input_output_aliases={8: 2, 9: 3, 10: 4},
        compiler_params=params(),
        cost_estimate=cost(5),
        name="last",
    )(plan, from_5, *stats, slope_r, slope_c, order, *sums)[:2]
    return grad[None], disp[:, None]


def solution(mesh):
    return jax.shard_map(
        per_device,
        mesh=mesh,
        in_specs=(
            P("sec", "strip", None),
            P("sec", None, "strip"),
            P("sec", "strip"),
            P("sec", None, None),
            P("sec"),
            P(),
        ),
        out_specs=(P("sec", "strip", None), P(None, "sec", "strip", None)),
        check_vma=False,
    )
```

```python
import functools

import jax
import jax.numpy as jnp
from jax import lax
from jax.experimental import pallas as pl
from jax.experimental.pallas import tpu as pltpu
from jax.sharding import PartitionSpec as P


TAPS = 4
HALO = 12
STEPS = 19
SUBS = 8
EXT = STEPS * SUBS
TILES = 8
CELLS = 81.0
F32 = jnp.float32
BF16 = jnp.bfloat16
VMEM = pl.BlockSpec(memory_space=pltpu.VMEM)
SMEM = pl.BlockSpec(memory_space=pltpu.SMEM)
HBM = pl.BlockSpec(memory_space=pl.ANY)
EDGE = 24
UNROLL = 3
GROUP = 8
BLOCK = 24


def window_sums(seq, width):
    count = len(seq) - width + 1
    out = [None] * count
    for base in range(0, count, width):
        suffix = [None] * width
        suffix[width - 1] = seq[base + width - 1]
        for i in range(width - 2, -1, -1):
            suffix[i] = seq[base + i] + suffix[i + 1]
        prefix = None
        for i in range(width):
            if base + i >= count:
                break
            if i == 0:
                out[base] = suffix[0]
            else:
                nxt = seq[base + width + i - 1]
                prefix = nxt if prefix is None else prefix + nxt
                out[base + i] = suffix[i] + prefix
    return out


def row_window(steps):
    low = [pltpu.roll(v, 1, 0) for v in steps[-4:]]
    high = [pltpu.roll(v, SUBS - 1, 0) for v in steps[:4]]
    return window_sums(low + steps + high, 9)


def col_window(seq):
    suffix = [None] * 8
    suffix[7] = seq[7]
    for i in range(6, -1, -1):
        suffix[i] = seq[i] + suffix[i + 1]
    out = []
    prefix = None
    for i in range(8):
        prefix = seq[8 + i] if prefix is None else prefix + seq[8 + i]
        out.append(suffix[i] + prefix)
    return out


def steps_of(value):
    return [value[8 * k : 8 * k + 8] for k in range(STEPS)]


def put_rows(ref, tile, values):
    for k, v in enumerate(values):
        ref[tile, 8 * k : 8 * k + 8, :] = v


def over_tiles(body, each=GROUP):
    lane = lax.broadcasted_iota(jnp.int32, (8, 128), 1)

    def turn_to(shift, edge):
        keep = lane != edge
        return lambda v: jnp.where(keep, pltpu.roll(v, shift, 1), 0.0)

    if each == TILES:
        for m in range(TILES):
            body(m, turn_to(127, 127) if m < 4 else turn_to(1, 0))
        return

    def part(q, carry):
        low = each * q < 4
        turn = turn_to(jnp.where(low, 127, 1), jnp.where(low, 127, 0))
        for i in range(each):
            body(each * q + i, turn)
        return carry

    lax.fori_loop(0, TILES // each, part, 0)


def put_box(pair, m, turn, values):
    main, side = pair
    sums = row_window(values)
    put_rows(side, m, [turn(v) for v in sums])
    put_rows(main, m, sums)


def get_box(pair, at):
    main, side = pair
    rows = pl.ds(at, 8)
    seq = [side[m, rows, :] for m in range(4, 8)]
    seq += [main[m, rows, :] for m in range(8)]
    seq += [side[m, rows, :] for m in range(4)]
    return col_window(seq)


def over_steps(body, each=UNROLL):
    def step(i, carry):
        for e in range(each):
            k = each * i + e
            body(k, pl.multiple_of(8 * k, 8))
        return carry

    lax.fori_loop(0, STEPS // each, step, 0)
    for k in range(STEPS // each * each, STEPS):
        body(k, 8 * k)


def split3(value):
    hi = value.astype(BF16).astype(F32)
    rest = value - hi
    mid = rest.astype(BF16).astype(F32)
    return hi, mid, rest - mid


def exchange_stage(source, target, lead, bit, blocks, first, each):
    lane = lax.broadcasted_iota(jnp.int32, (8, 128), 1)
    span = 16 << bit
    upper = (lane & span) != 0

    def step(s, carry):
        for e in range(each):
            at = pl.ds(pl.multiple_of(8 * (s * each + e), 8) + first, 8)
            for which in lead:
                for m in range(TILES):
                    if m & (1 << bit):
                        continue
                    lo, hi = which + (m, at), which + (m | (1 << bit), at)
                    a, b = source[lo], source[hi]
                    target[lo] = jnp.where(upper, pltpu.roll(b, span, 1), a)
                    target[hi] = jnp.where(upper, b, pltpu.roll(a, 128 - span, 1))
        return carry

    lax.fori_loop(0, blocks // each, step, 0)


def to_blocked(work, other, blocks):
    exchange_stage(work, other, [()], 0, blocks, 0, blocks)
    exchange_stage(other, work, [()], 1, blocks, 0, blocks)
    exchange_stage(work, other, [()], 2, blocks, 0, blocks)


def grouped_lanes():
    lane = lax.broadcasted_iota(jnp.int32, (8, 128), 1)
    return 8 * (lane % 16) + lane // 16


def table_rows(line, shift, tap):
    row = lax.broadcasted_iota(jnp.int32, (8, 128), 0)
    hi, mid, lo = split3(pltpu.roll(line, HALO, 1))
    zero = jnp.zeros((8, 128), F32)
    full = jnp.where(row == 0, hi, jnp.where(row == 1, mid, jnp.where(row == 2, lo, zero)))
    if tap == 0:
        full = jnp.where(row == 3, shift, full)
    return full


def halo_kernel(shift_ref, img_hbm, weights_hbm, first_ref, second_ref, edge, weights, work, other, sems):
    moves = [
        pltpu.make_async_copy(img_hbm.at[0, pl.ds(0, EDGE)], edge.at[0], sems.at[0]),
        pltpu.make_async_copy(img_hbm.at[0, pl.ds(128 - EDGE, EDGE)], edge.at[1], sems.at[1]),
        pltpu.make_async_copy(weights_hbm.at[0], weights, sems.at[2]),
    ]
    for move in moves:
        move.start()
    for move in moves:
        move.wait()
    pick = grouped_lanes()
    for j in range(TILES):
        for side in range(2):
            tile = edge[side, :, 128 * j : 128 * j + 128].astype(F32)
            for b in range(3):
                work[j, 24 * side + 8 * b : 24 * side + 8 * b + 8, :] = jnp.take_along_axis(
                    tile[8 * b : 8 * b + 8], pick, axis=1
                )
    to_blocked(work, other, 6)
    lane = lax.broadcasted_iota(jnp.int32, (8, 128), 1)
    zero = jnp.zeros((8, 128), F32)
    shift = jnp.full((8, 128), shift_ref[0, 0], jnp.int32).astype(F32)
    even = lax.axis_index("strip") % 2 == 0

    row = lax.broadcasted_iota(jnp.int32, (8, 128), 0)
    tables = [table_rows(jnp.broadcast_to(weights[tap : tap + 1, :], (8, 128)), shift, tap) for tap in range(TAPS)]

    def fill(up_ref, down_ref):
        for m in range(TILES):
            cols = slice(128 * m, 128 * m + 128)
            table = tables[m // 2]
            before = jnp.where(lane < HALO, table, zero) if m % 2 == 0 else zero
            after = jnp.where((lane >= HALO) & (lane < 2 * HALO), table, zero) if m % 2 else zero
            up_0 = jnp.where(row < 4, before, other[m, EDGE : EDGE + 8, :])
            down_2 = jnp.where(row >= 4, pltpu.roll(after, 4, 0), other[m, 16:24, :])
            up_ref[:, cols] = jnp.concatenate([up_0, other[m, EDGE + 8 : 2 * EDGE, :]], axis=0).astype(BF16)
            down_ref[:, cols] = jnp.concatenate([other[m, 0:16, :], down_2], axis=0).astype(BF16)

    @pl.when(even)
    def _():
        fill(first_ref, second_ref)

    @pl.when(jnp.logical_not(even))
    def _():
        fill(second_ref, first_ref)


def prep_kernel(img_ref, small_ref, own_ref, img_out, taps_out, order, work, other):
    order[...] = column_order()
    shift = jnp.broadcast_to(small_ref[8:9, 0:128], (8, 128))
    lane = lax.broadcasted_iota(jnp.int32, (8, 128), 1)
    zero = jnp.zeros((8, 128), F32)
    pick = grouped_lanes()
    for j in range(TILES):
        cols = slice(128 * j, 128 * j + 128)
        tile = img_ref[:, cols].astype(F32)
        for b in range(16):
            work[j, 8 * b : 8 * b + 8, :] = jnp.take_along_axis(tile[8 * b : 8 * b + 8], pick, axis=1)
        work[j, 128:136, :] = jnp.take_along_axis(small_ref[0:8, cols], pick, axis=1)
    to_blocked(work, other, 17)
    for m in range(TILES):
        img_out[:, 128 * m : 128 * m + 128] = other[m, 0:128, :].astype(BF16)
        taps_out[m] = other[m, 128:136, :]
    for tap in range(TAPS):
        line = jnp.broadcast_to(small_ref[4 + tap : 5 + tap, 0:128], (8, 128))
        full = table_rows(line, shift, tap)
        at = 256 * tap
        own_ref[:, at : at + 128] = jnp.where(lane >= HALO, full, zero).astype(BF16)
        own_ref[:, at + 128 : at + 256] = jnp.where(lane < HALO, full, zero).astype(BF16)


def warp_kernel(shift_ref, img_ref, first_ref, second_ref, own_ref, taps_ref, out_ref, row_warped, virtual):
    even = lax.axis_index("strip") % 2 == 0
    first, second = first_ref[...].astype(F32), second_ref[...].astype(F32)
    low = jnp.where(even, second, first)
    high = jnp.where(even, first, second)
    meta = (low[0:8] + own_ref[...].astype(F32) + pltpu.roll(high[16:24], 4, 0)).astype(BF16)
    place = lax.broadcasted_iota(jnp.int32, (EXT, 256), 0)
    rho = (place % 8) * STEPS + place // 8
    spread = jnp.where(
        rho == lax.broadcasted_iota(jnp.int32, (EXT, 256), 1), jnp.float32(1), jnp.float32(0)
    ).astype(BF16)
    columns = [
        lax.dot_general(
            spread,
            meta[:, 256 * tap : 256 * tap + 256],
            (((1,), (1,)), ((), ())),
            preferred_element_type=F32,
        )
        for tap in range(TAPS)
    ]
    width = 2 * BLOCK + 128
    lane = lax.broadcasted_iota(jnp.int32, (EXT, width), 1)
    image_row = jnp.where((lane >= 7) & (lane < EDGE + 128 + 18), lane - EDGE, 2000)
    own_row = lax.broadcasted_iota(jnp.int32, (EXT, width), 0)
    own_row = (own_row % 8) * STEPS + own_row // 8 - HALO
    offset = (image_row - own_row + 1).astype(F32) - columns[0][:, 3:4]
    value = jnp.zeros((EXT, width), F32)
    for tap in range(TAPS):
        weight = columns[tap][:, 0:1] + columns[tap][:, 1:2] + columns[tap][:, 2:3]
        value = jnp.where(offset == float(tap), weight, value)
    hi, mid, lo = split3(value)
    source = jnp.concatenate([low, img_ref[...].astype(F32), high], axis=0).astype(BF16)
    total = jnp.zeros((EXT, 1024), F32)
    for piece in (lo, mid, hi):
        total = total + jnp.dot(piece.astype(BF16), source, preferred_element_type=F32)
    rounded = total.astype(BF16).astype(F32)
    for m in range(TILES):
        row_warped[m] = rounded[:, 128 * m : 128 * m + 128]
    first = shift_ref[0] - 1
    lane = lax.broadcasted_iota(jnp.int32, (EXT, 128), 1)
    for v in range(TILES + TAPS - 1):
        column = first + v
        tile = lax.bitwise_and(column, 7)
        far = lax.shift_right_arithmetic(column, 3)
        moved = pltpu.roll(row_warped[tile], lax.bitwise_and(-far, 127), 1)
        virtual[v] = jnp.where((lane + far >= 0) & (lane + far < 128), moved, 0.0)
    for m in range(TILES):
        terms = [taps_ref[m, t : t + 1, :] * virtual[m + t] for t in range(TAPS)]
        out_ref[m] = ((terms[0] + terms[1]) + (terms[2] + terms[3])).astype(BF16)


def inside_rows(k, plan):
    rho = (lax.broadcasted_iota(jnp.int32, (8, 128), 0) * STEPS + k).astype(F32)
    return (rho >= plan[6:7, :]) & (rho < plan[7:8, :])


def own_stats(x_ref, plan, x_wide, sum_x, root_x, slope_r, slope_c, boxes):
    def rows(m, turn):
        value = x_ref[m].astype(F32)
        x_wide[m] = value
        steps = steps_of(value)
        put_box(boxes[0], m, turn, steps)
        put_box(boxes[1], m, turn, steps_of(value * value))
        put_rows(boxes[2][1], m, [turn(v) for v in steps])
        seq = [pltpu.roll(steps[-1], 1, 0)] + steps + [pltpu.roll(steps[0], SUBS - 1, 0)]
        put_rows(slope_r, m, [(seq[k + 2] - seq[k]) for k in range(STEPS)])

    over_tiles(rows)

    def cols(k, at):
        s1 = get_box(boxes[0], at)
        s2 = get_box(boxes[1], at)
        scale = jnp.where(inside_rows(k, plan), -0.5 / 9.0, 0.0)
        rows = pl.ds(at, 8)
        x = [boxes[2][1][7, rows, :]] + [x_wide[m, rows, :] for m in range(8)] + [boxes[2][1][0, rows, :]]
        for m in range(TILES):
            sum_x[m, rows, :] = s1[m]
            root_x[m, rows, :] = lax.rsqrt(s2[m] - s1[m] * s1[m] * (1.0 / CELLS) + 0.25 * CELLS)
            slope_r[m, rows, :] = slope_r[m, rows, :] * scale
            slope_c[m, rows, :] = (x[m + 2] - x[m]) * scale

    over_steps(cols)


def add_pair(y_ref, which, plan, first, x_wide, sum_x, root_x, sum_g, sum_h, sum_t, y_wide, coef, boxes):
    def rows(m, turn):
        value = y_ref[m].astype(F32)
        y_wide[m] = value
        steps = steps_of(value)
        turned = [turn(v) for v in steps]
        put_rows(boxes[0][0], m, row_window(steps))
        put_rows(boxes[1][0], m, row_window([v * v for v in steps]))
        put_rows(boxes[0][1], m, row_window(turned))
        put_rows(boxes[1][1], m, row_window([v * v for v in turned]))
        put_box(boxes[2], m, turn, steps_of(value * x_wide[m]))

    over_tiles(rows)

    def cols(k, at):
        scale = jnp.where(inside_rows(k, plan), plan[which : which + 1, :], 0.0)
        s1 = get_box(boxes[0], at)
        s2 = get_box(boxes[1], at)
        s3 = get_box(boxes[2], at)
        for m in range(TILES):
            here = (m, pl.ds(at, 8), slice(None))
            mean = s1[m] * (1.0 / CELLS)
            root = lax.rsqrt(s2[m] - s1[m] * mean + 0.25 * CELLS)
            cov = s3[m] - sum_x[here] * mean
            u = scale * root_x[here] * root
            coef[here] = u
            g, h = u * cov, u * s1[m]
            sum_g[here] = g if first else sum_g[here] + g
            sum_h[here] = h if first else sum_h[here] + h

    over_steps(cols)

    def rows_2(m, turn):
        put_box(boxes[0], m, turn, steps_of(coef[m]))

    over_tiles(rows_2)

    def cols_2(k, at):
        s1 = get_box(boxes[0], at)
        for m in range(TILES):
            here = (m, pl.ds(at, 8), slice(None))
            t = y_wide[here] * s1[m]
            sum_t[here] = t if first else sum_t[here] + t

    over_steps(cols_2)


def column_order():
    source = lax.broadcasted_iota(jnp.int32, (512, 512), 0)
    column = lax.broadcasted_iota(jnp.int32, (512, 512), 1)
    tile = 4 * ((source // 64) % 2) + source // 128
    return jnp.where(8 * (source % 64) + tile == column, 1.0, 0.0).astype(BF16)


def restore(natural, order, which, target):
    lane = lax.broadcasted_iota(jnp.int32, (128, 128), 1)
    upper = lane >= 64
    rows = slice(HALO, HALO + 128)
    for w in which:
        halves = [], []
        for m in range(4):
            a, b = natural[w, m, rows, :], natural[w, m + 4, rows, :]
            halves[0].append(jnp.where(upper, pltpu.roll(b, 64, 1), a))
            halves[1].append(jnp.where(upper, b, pltpu.roll(a, 64, 1)))
        for h in range(2):
            value = jnp.concatenate(halves[h], axis=1)
            hi = value.astype(BF16)
            lo = (value - hi.astype(F32)).astype(BF16)
            target[w, :, 512 * h : 512 * h + 512] = jnp.dot(
                hi, order[...], preferred_element_type=F32
            ) + jnp.dot(lo, order[...], preferred_element_type=F32)


def finish(x_wide, sum_x, root_x, slope_r, slope_c, sum_g, sum_h, sum_t, natural, order, wide, sems, grad_hbm, disp_hbm, boxes):
    def rows(m, turn):
        root = root_x[m]
        g = root * root * sum_g[m]
        put_box(boxes[0], m, turn, steps_of(sum_h[m] - g * sum_x[m]))
        put_box(boxes[1], m, turn, steps_of(g))

    over_tiles(rows)

    def cols(k, at):
        s1 = get_box(boxes[0], at)
        s2 = get_box(boxes[1], at)
        for m in range(TILES):
            here = (m, pl.ds(at, 8), slice(None))
            grad = s1[m] * (1.0 / CELLS) + x_wide[here] * s2[m] - sum_t[here]
            natural[0, m, pl.ds(k, 8, stride=STEPS), :] = grad
            sum_g[here] = grad * slope_r[here]
            sum_h[here] = grad * slope_c[here]

    over_steps(cols)
    restore(natural, order, [0], wide)
    out = pltpu.make_async_copy(wide.at[0], grad_hbm, sems.at[0])
    out.start()

    def rows_2(m, turn):
        put_box(boxes[0], m, turn, steps_of(sum_g[m]))
        put_box(boxes[1], m, turn, steps_of(sum_h[m]))

    over_tiles(rows_2)

    def cols_2(k, at):
        s1 = get_box(boxes[0], at)
        s2 = get_box(boxes[1], at)
        for m in range(TILES):
            natural[1, m, pl.ds(k, 8, stride=STEPS), :] = s1[m]
            natural[2, m, pl.ds(k, 8, stride=STEPS), :] = s2[m]

    over_steps(cols_2)
    restore(natural, order, [1, 2], wide)
    out_2 = pltpu.make_async_copy(wide.at[pl.ds(1, 2)], disp_hbm, sems.at[1])
    out_2.start()
    out.wait()
    out_2.wait()


def others(own):
    way = 1 - 2 * (own % 2)
    return [own + way, own + 2 * way, own - way, own - 2 * way, own - 3 * way, own + 3 * way]


def field():
    return pltpu.VMEM((TILES, EXT, 128), F32)


def shape(dims, kind):
    return jax.ShapeDtypeStruct(dims, kind)


FIELD = shape((TILES, EXT, 128), F32)


def own_kernel(small, x, x_wide, sum_x, root_x, slope_r, slope_c, plan, *boxes):
    own, strip = lax.axis_index("sec"), lax.axis_index("strip")
    row = lax.broadcasted_iota(jnp.int32, (8, 128), 0)
    lane = lax.broadcasted_iota(jnp.int32, (8, 128), 1)
    table = small[8:16, 0:128]
    lines = jnp.where(row == 6, jnp.where(strip == 0, HALO, 0), jnp.where(strip == 15, HALO + 128, EXT)).astype(F32)
    for i, section in enumerate(others(own)):
        low, gap = jnp.minimum(own, section), jnp.abs(own - section)
        here = (row == gap) & (lane == low) & (section >= 0) & (section < 16)
        weight = jnp.sum(jnp.sum(jnp.where(here, table, 0.0), axis=1, keepdims=True), axis=0, keepdims=True)
        lines = jnp.where(row == i, weight, lines)
    plan[...] = lines
    own_stats(x, lines, x_wide, sum_x, root_x, slope_r, slope_c, paired(boxes))


def paired(refs):
    return [(refs[2 * i], refs[2 * i + 1]) for i in range(3)]


def pair_kernel(turns, plan, *refs):
    ys, refs = refs[: len(turns)], refs[len(turns) :]
    first = 0 in turns
    kept = 0 if first else 3
    x_wide, sum_x, root_x = refs[:3]
    g, h, t = refs[3 + kept : 6 + kept]
    y_wide, coef = refs[6 + kept : 8 + kept]
    boxes = paired(refs[8 + kept :])
    for i, y in zip(turns, ys):
        add_pair(y, i, plan[...], i == 0, x_wide, sum_x, root_x, g, h, t, y_wide, coef, boxes)


def last_kernel(turns, plan, *refs):
    ys, refs = refs[: len(turns)], refs[len(turns) :]
    x_wide, sum_x, root_x, slope_r, slope_c, order, _, _, _, grad, disp, g, h, t, y_wide, coef, natural, wide, sems = refs[:19]
    boxes = paired(refs[19:])
    for i, y in zip(turns, ys):
        add_pair(y, i, plan[...], False, x_wide, sum_x, root_x, g, h, t, y_wide, coef, boxes)
    finish(x_wide, sum_x, root_x, slope_r, slope_c, g, h, t, natural, order, wide, sems, grad, disp, boxes)


def last_scratch():
    three = pltpu.VMEM((3, TILES, EXT, 128), F32)
    wide = pltpu.VMEM((3, 128, 1024), F32)
    return [field(), field(), three, wide, pltpu.SemaphoreType.DMA((2,))] + [field() for _ in range(6)]


def params(mib=24):
    return pltpu.CompilerParams(vmem_limit_bytes=mib * 1024 * 1024)


def cost(us):
    return pl.CostEstimate(flops=int(us * 4_000_000), bytes_accessed=1_000_000, transcendentals=0)


def add_pairs(turns, plan, ys, stats, sums):
    ins = [plan, *ys, *stats, *sums]
    start = len(ins) - len(sums)
    return pl.pallas_call(
        functools.partial(pair_kernel, turns),
        out_shape=(FIELD,) * 3,
        in_specs=[VMEM] * len(ins),
        out_specs=(VMEM,) * 3,
        scratch_shapes=[field() for _ in range(8)],
        input_output_aliases={start + i: i for i in range(len(sums))},
        compiler_params=params(),
        cost_estimate=cost(1.5 * len(turns)),
        name="pair",
    )(*ins)


def per_device(images, row_weights, row_shift, col_weights, col_shift, pair_on):
    block = shape((BLOCK, 1024), BF16)

    def wide(value):
        return jnp.pad(value.astype(F32), ((0, 0), (0, 1024 - value.shape[1])))

    small = jnp.concatenate(
        [
            col_weights[0].astype(F32),
            wide(row_weights[0]),
            jnp.broadcast_to(row_shift.astype(F32), (1, 1024)),
            wide(pair_on.T),
            jnp.zeros((4, 1024), F32),
        ]
    )
    halo = pl.pallas_call(
        halo_kernel,
        out_shape=(block, block),
        in_specs=[SMEM, HBM, HBM],
        out_specs=(VMEM,) * 2,
        scratch_shapes=[
            pltpu.VMEM((2, EDGE, 1024), BF16),
            pltpu.VMEM((TAPS, 128), F32),
            pltpu.VMEM((TILES, 48, 128), F32),
            pltpu.VMEM((TILES, 48, 128), F32),
            pltpu.SemaphoreType.DMA((3,)),
        ],
        compiler_params=pltpu.CompilerParams(vmem_limit_bytes=66_500_000),
        name="halo",
    )(row_shift, images, row_weights)
    strips = range(16)

    def swap(value, step):
        pairs = [(s, s + step * (1 - 2 * (s % 2))) for s in strips]
        return lax.ppermute(value, "strip", [p for p in pairs if 0 <= p[1] < 16])

    first = swap(halo[0], 1)
    second = swap(halo[1], -1)
    own, image, taps, order = pl.pallas_call(
        prep_kernel,
        out_shape=(
            shape((8, 1024), BF16),
            shape((128, 1024), BF16),
            shape((TILES, 8, 128), F32),
            shape((512, 512), BF16),
        ),
        in_specs=[VMEM] * 2,
        out_specs=(VMEM,) * 4,
        scratch_shapes=[pltpu.VMEM((TILES, 136, 128), F32)] * 2,
        compiler_params=params(),
        cost_estimate=cost(1),
        name="prep",
    )(images[0], small)
    warped = pl.pallas_call(
        warp_kernel,
        out_shape=shape((TILES, EXT, 128), BF16),
        in_specs=[SMEM] + [VMEM] * 5,
        out_specs=VMEM,
        scratch_shapes=[field(), pltpu.VMEM((TILES + TAPS - 1, EXT, 128), F32)],
        compiler_params=params(),
        name="warp",
    )(col_shift, image, first, second, own, taps)
    sections = range(16)

    def send(value, target):
        pairs = [(s, target(s, 1 - 2 * (s % 2))) for s in sections]
        return lax.ppermute(value, "sec", [p for p in pairs if 0 <= p[1] < 16])

    from_0 = send(warped, lambda s, way: s + way)
    from_1 = send(warped, lambda s, way: s - 2 * way)
    from_2 = send(from_1, lambda s, way: s + way)
    from_3 = send(warped, lambda s, way: s + 2 * way)
    from_4 = send(from_1, lambda s, way: s - way)
    from_5 = send(from_3, lambda s, way: s + way)
    x_wide, sum_x, root_x, slope_r, slope_c, plan = pl.pallas_call(
        own_kernel,
        out_shape=(FIELD,) * 5 + (shape((8, 128), F32),),
        in_specs=[VMEM, VMEM],
        out_specs=(VMEM,) * 6,
        scratch_shapes=[field() for _ in range(6)],
        compiler_params=params(),
        cost_estimate=cost(1.3),
        name="own",
    )(small, warped)
    stats = (x_wide, sum_x, root_x)
    sums = ()
    for i, y in enumerate((from_0, from_1, from_2, from_3, from_4)):
        sums = add_pairs((i,), plan, (y,), stats, sums)
    grad, disp = pl.pallas_call(
        functools.partial(last_kernel, (5,)),
        out_shape=(shape((128, 1024), F32), shape((2, 128, 1024), F32)) + (FIELD,) * 3,
        in_specs=[VMEM] * 11,
        out_specs=(HBM, HBM) + (VMEM,) * 3,
        scratch_shapes=last_scratch(),
        input_output_aliases={8: 2, 9: 3, 10: 4},
        compiler_params=params(),
        cost_estimate=cost(5),
        name="last",
    )(plan, from_5, *stats, slope_r, slope_c, order, *sums)[:2]
    return grad[None], disp[:, None]


def solution(mesh):
    return jax.shard_map(
        per_device,
        mesh=mesh,
        in_specs=(
            P("sec", "strip", None),
            P("sec", None, "strip"),
            P("sec", "strip"),
            P("sec", None, None),
            P("sec"),
            P(),
        ),
        out_specs=(P("sec", "strip", None), P(None, "sec", "strip", None)),
        check_vma=False,
    )
```
